8 devices in a mesh: dp: 1 (over z), tp: 2 (over y), sp: 4 (over x, core).
Axes of the slice: x: 2, y: 2, z: 1, core: 2. Of those that a mesh axis runs over, the one named last changes fastest.
Arguments:
- hidden: bfloat16 [256, 6144], P('dp')
- lat_cache: bfloat16 [256, 2048, 512], P('dp', 'sp')
- rope_cache: bfloat16 [256, 2048, 64], P('dp', 'sp')
- positions: int32 [256], P('dp')
- w_dq: bfloat16 [6144, 1536], replicated
- gain_q: bfloat16 [1536], replicated
- w_dkv: bfloat16 [6144, 576], replicated
- gain_kv: bfloat16 [512], replicated
- w_uq: bfloat16 [1536, 64, 192], P(None, 'tp')
- w_uk: bfloat16 [512, 64, 128], P(None, 'tp')
- w_uv: bfloat16 [512, 64, 128], P(None, 'tp')
- w_out: bfloat16 [8192, 6144], P('tp')
Outputs:
- output 1: bfloat16 [256, 6144], P('dp')
- output 2: bfloat16 [256, 2048, 512], P('dp', 'sp')
- output 3: bfloat16 [256, 2048, 64], P('dp', 'sp')
All inputs are finite; a program needn't handle non-finite values.
Results may differ from the reference program's by a relative error of at most 0.0116176.
Values sent between devices are 32-bit elements.
A program may use at most 1.75 GiB of HBM per device.

```python
import math
import jax
import jax.numpy as jnp
from jax import lax

BATCH = 256
SEQ = 2048
DMODEL = 6144
HEADS = 64
QRANK = 1536
KVRANK = 512
NOPE = 128
ROPE = 64
VHEAD = 128

EPSILON = 1e-6
ROPE_BASE = 50000.0
SCORE_SCALE = (1.0 + 0.1 * math.log(32.0)) ** 2 / math.sqrt(NOPE + ROPE)
LAT_SPREAD = 1.2
ROPE_SPREAD = 1.7


def setup_inputs(seed: int = 0, part: int = 0) -> dict:
    base_key = jax.random.key(seed)
    shared_keys = jax.random.split(base_key, 8)
    part_keys = jax.random.split(jax.random.fold_in(base_key, part), 5)
    hidden = jax.random.normal(part_keys[0], (BATCH, DMODEL), jnp.float32)
    lat_cache = LAT_SPREAD * jax.random.normal(part_keys[1], (BATCH, SEQ, KVRANK), jnp.float32)
    rope_cache = ROPE_SPREAD * jax.random.normal(part_keys[2], (BATCH, SEQ, ROPE), jnp.float32)
    long_pos = jax.random.randint(part_keys[3], (BATCH,), 0, SEQ, jnp.int32)
    short_pos = jax.random.randint(part_keys[4], (BATCH,), 0, 4, jnp.int32)
    positions = jnp.where(jnp.arange(BATCH) % 4 == 1, short_pos, long_pos)
    positions = positions.at[0].set(SEQ - 1).at[1].set(0)
    w_dq = jax.random.normal(shared_keys[0], (DMODEL, QRANK), jnp.float32) * DMODEL ** -0.5
    gain_q = 1.0 + 0.5 * jax.random.normal(shared_keys[1], (QRANK,), jnp.float32)
    w_dkv = jax.random.normal(shared_keys[2], (DMODEL, KVRANK + ROPE), jnp.float32) * DMODEL ** -0.5
    gain_kv = 1.0 + 0.5 * jax.random.normal(shared_keys[3], (KVRANK,), jnp.float32)
    w_uq = jax.random.normal(shared_keys[4], (QRANK, HEADS, NOPE + ROPE), jnp.float32) * QRANK ** -0.5
    w_uk = jax.random.normal(shared_keys[5], (KVRANK, HEADS, NOPE), jnp.float32) * KVRANK ** -0.5
    w_uv = jax.random.normal(shared_keys[6], (KVRANK, HEADS, VHEAD), jnp.float32) * KVRANK ** -0.5
    w_out = jax.random.normal(shared_keys[7], (HEADS * VHEAD, DMODEL), jnp.float32) * (HEADS * VHEAD) ** -0.5
    return {
        'hidden': hidden.astype(jnp.bfloat16),
        'lat_cache': lat_cache.astype(jnp.bfloat16),
        'rope_cache': rope_cache.astype(jnp.bfloat16),
        'positions': positions,
        'w_dq': w_dq.astype(jnp.bfloat16),
        'gain_q': gain_q.astype(jnp.bfloat16),
        'w_dkv': w_dkv.astype(jnp.bfloat16),
        'gain_kv': gain_kv.astype(jnp.bfloat16),
        'w_uq': w_uq.astype(jnp.bfloat16),
        'w_uk': w_uk.astype(jnp.bfloat16),
        'w_uv': w_uv.astype(jnp.bfloat16),
        'w_out': w_out.astype(jnp.bfloat16),
    }


def rms_norm(values, gain):
    vals32 = values.astype(jnp.float32)
    inv_rms = lax.rsqrt(jnp.mean(vals32 * vals32, axis=-1, keepdims=True) + EPSILON)
    return vals32 * inv_rms * gain.astype(jnp.float32)


def rope_angles(positions):
    half_dim = ROPE // 2
    inv_freq = ROPE_BASE ** (-jnp.arange(half_dim).astype(jnp.float32) / half_dim)
    return positions.astype(jnp.float32)[:, None] * inv_freq[None, :]


def rotate_pairs(values, cos_t, sin_t):
    half_dim = values.shape[-1] // 2
    first_half = values[..., :half_dim]
    second_half = values[..., half_dim:]
    return jnp.concatenate([first_half * cos_t - second_half * sin_t, second_half * cos_t + first_half * sin_t], axis=-1)


def attend_one(operands):
    q_abs, q_rope, lat_all, rope_all, position = operands
    lat32 = lat_all.astype(jnp.float32)
    scores = (jnp.einsum('hk,sk->hs', q_abs.astype(jnp.float32), lat32) + jnp.einsum('hr,sr->hs', q_rope.astype(jnp.float32), rope_all.astype(jnp.float32))) * SCORE_SCALE
    key_valid = jnp.arange(SEQ)[None, :] <= position
    scores = jnp.where(key_valid, scores, -jnp.inf)
    probs = jax.nn.softmax(scores, axis=-1)
    return jnp.einsum('hs,sk->hk', probs, lat32).astype(jnp.bfloat16)


def reference(hidden, lat_cache, rope_cache, positions, w_dq, gain_q, w_dkv, gain_kv, w_uq, w_uk, w_uv, w_out):
    angles = rope_angles(positions)
    cos_t = jnp.cos(angles)
    sin_t = jnp.sin(angles)
    h_q = jnp.dot(hidden, w_dq, preferred_element_type=jnp.float32).astype(jnp.bfloat16)
    c_q = rms_norm(h_q, gain_q).astype(jnp.bfloat16)
    q_full = jnp.einsum('br,rhd->bhd', c_q.astype(jnp.float32), w_uq.astype(jnp.float32)).astype(jnp.bfloat16)
    q_nope = q_full[:, :, :NOPE]
    q_rope = rotate_pairs(q_full[:, :, NOPE:].astype(jnp.float32), cos_t[:, None, :], sin_t[:, None, :]).astype(jnp.bfloat16)
    kv_down = jnp.dot(hidden, w_dkv, preferred_element_type=jnp.float32).astype(jnp.bfloat16)
    lat_new = rms_norm(kv_down[:, :KVRANK], gain_kv).astype(jnp.bfloat16)
    rope_new = rotate_pairs(kv_down[:, KVRANK:].astype(jnp.float32), cos_t, sin_t).astype(jnp.bfloat16)
    slot_hit = (jnp.arange(SEQ)[None, :] == positions[:, None])[:, :, None]
    lat_all = jnp.where(slot_hit, lat_new[:, None, :], lat_cache)
    rope_all = jnp.where(slot_hit, rope_new[:, None, :], rope_cache)
    q_abs = jnp.einsum('bhn,khn->bhk', q_nope.astype(jnp.float32), w_uk.astype(jnp.float32)).astype(jnp.bfloat16)
    o_lat = lax.map(attend_one, (q_abs, q_rope, lat_all, rope_all, positions))
    o_heads = jnp.einsum('bhk,khv->bhv', o_lat.astype(jnp.float32), w_uv.astype(jnp.float32)).astype(jnp.bfloat16)
    attn_out = jnp.dot(o_heads.reshape(BATCH, HEADS * VHEAD), w_out, preferred_element_type=jnp.float32)
    return (hidden.astype(jnp.float32) + attn_out).astype(jnp.bfloat16), lat_all, rope_all
```

```python
import functools
import math
import jax
import jax.numpy as jnp
from jax import lax
from jax.experimental import pallas as pl
from jax.experimental.pallas import tpu as pltpu
from jax.sharding import PartitionSpec as P

EPSILON = 1e-6
ROPE_BASE = 50000.0
YARN_MSCALE = 1.0 + 0.1 * math.log(32.0)
MASK_VALUE = -1e30
GROUP = 4
RING = 8
AHEAD = 4


def rms_norm(values, gain):
    vals32 = values.astype(jnp.float32)
    inv_rms = lax.rsqrt(jnp.mean(vals32 * vals32, axis=-1, keepdims=True) + EPSILON)
    return vals32 * inv_rms * gain.astype(jnp.float32)


def rope_tables(positions, rope_dim):
    half_dim = rope_dim // 2
    inv_freq = ROPE_BASE ** (-jnp.arange(half_dim).astype(jnp.float32) / half_dim)
    angles = positions.astype(jnp.float32)[:, None] * inv_freq[None, :]
    return jnp.cos(angles), jnp.sin(angles)


def rotate_pairs(values, cos_t, sin_t):
    half_dim = values.shape[-1] // 2
    first_half = values[..., :half_dim]
    second_half = values[..., half_dim:]
    return jnp.concatenate([first_half * cos_t - second_half * sin_t, second_half * cos_t + first_half * sin_t], axis=-1)


def heads_kernel(cq_ref, cos_ref, sin_ref, wuq_ref, wuk_ref, qa_ref, qr_ref, wide, lines, rlines):
    block = wuq_ref.shape[0]
    nope = wuk_ref.shape[2]
    rank = wuk_ref.shape[0]
    rdim = wuq_ref.shape[1] - nope
    hdim = rdim // 2
    wide[...] = wuk_ref[...].astype(jnp.float32)
    cq = cq_ref[...]
    cos = cos_ref[...]
    sin = sin_ref[...]
    for h in range(block):
        q = lax.dot_general(cq, wuq_ref[h], (((1,), (1,)), ((), ())), preferred_element_type=jnp.float32).astype(jnp.bfloat16)
        r = q[:, nope:].astype(jnp.float32)
        turned = jnp.concatenate([-r[:, hdim:], r[:, :hdim]], axis=1)
        rlines[:, h, :rdim] = r * cos + turned * sin
        wk = wide[:, h, :].astype(jnp.bfloat16)
        lines[:, h, :rank] = lax.dot_general(q[:, :nope], wk, (((1,), (1,)), ((), ())), preferred_element_type=jnp.float32)
    qa_ref[...] = lines[:, :, :rank].astype(jnp.bfloat16)
    qr_ref[...] = rlines[:, :, :rdim].astype(jnp.bfloat16)


def head_queries(cq, cos2, sin2, w_uq_t, w_uk):
    rows, qrank = cq.shape
    heads, qdim, _ = w_uq_t.shape
    rank, _, nope = w_uk.shape
    rdim = qdim - nope
    block = 8
    return pl.pallas_call(
        heads_kernel,
        grid=(heads // block,),
        in_specs=[
            pl.BlockSpec((rows, qrank), lambda i: (0, 0)),
            pl.BlockSpec((rows, rdim), lambda i: (0, 0)),
            pl.BlockSpec((rows, rdim), lambda i: (0, 0)),
            pl.BlockSpec((block, qdim, qrank), lambda i: (i, 0, 0)),
            pl.BlockSpec((rank, block, nope), lambda i: (0, i, 0)),
        ],
        out_specs=[
            pl.BlockSpec((rows, block, rank), lambda i: (0, i, 0)),
            pl.BlockSpec((rows, block, rdim), lambda i: (0, i, 0)),
        ],
        out_shape=[
            jax.ShapeDtypeStruct((rows, heads, rank), jnp.bfloat16),
            jax.ShapeDtypeStruct((rows, heads, rdim), jnp.bfloat16),
        ],
        scratch_shapes=[
            pltpu.VMEM((rank, block, nope), jnp.float32),
            pltpu.VMEM((rows, block, rank + 128), jnp.float32),
            pltpu.VMEM((rows, block, 128), jnp.float32),
        ],
        compiler_params=pltpu.CompilerParams(dimension_semantics=('arbitrary',), vmem_limit_bytes=48 * 2 ** 20),
        cost_estimate=pl.CostEstimate(flops=2 * rows * heads * (qdim * qrank + nope * rank), bytes_accessed=2 * heads * (qdim * qrank + nope * rank), transcendentals=0),
        name='head_queries',
    )(cq, cos2, sin2, w_uq_t, w_uk)


def project_inputs(hidden, positions, w_dq, gain_q, w_dkv, gain_kv, w_uq, w_uk):
    kv_rank = w_uk.shape[0]
    nope_dim = w_uk.shape[2]
    cos_t, sin_t = rope_tables(positions, w_uq.shape[2] - nope_dim)
    h_q = jnp.dot(hidden, w_dq, preferred_element_type=jnp.float32).astype(jnp.bfloat16)
    c_q = rms_norm(h_q, gain_q).astype(jnp.bfloat16)
    cos2 = jnp.concatenate([cos_t, cos_t], axis=1)
    sin2 = jnp.concatenate([sin_t, sin_t], axis=1)
    q_abs, q_rope = head_queries(c_q, cos2, sin2, jnp.transpose(w_uq, (1, 2, 0)), w_uk)
    kv_down = jnp.dot(hidden, w_dkv, preferred_element_type=jnp.float32).astype(jnp.bfloat16)
    lat_new = rms_norm(kv_down[:, :kv_rank], gain_kv).astype(jnp.bfloat16)
    rope_new = rotate_pairs(kv_down[:, kv_rank:].astype(jnp.float32), cos_t, sin_t).astype(jnp.bfloat16)
    return q_abs, q_rope, lat_new, rope_new


def attend_kernel(first, steps, scale, order_ref, pos_ref, where_ref, qa_ref, qr_ref, latn_ref, ropen_ref, lat_hbm, rope_hbm, *rest):
    uo_ref, us_ref, m_ref, l_ref, lat_out, rope_out, lat_buf, rope_buf, in_sem, out_sem = rest[-10:]
    t = pl.program_id(0)
    slots = lat_buf.shape[2]
    heads = qa_ref.shape[1]
    half = heads // 2
    start = where_ref[0]
    own = where_ref[1]

    def reads(step):
        ring = lax.rem(step, RING)
        out = []
        for g in range(GROUP):
            b = order_ref[first + step * GROUP + g]
            out.append(pltpu.make_async_copy(lat_hbm.at[b], lat_buf.at[ring, g], in_sem.at[ring, g, 0]))
            out.append(pltpu.make_async_copy(rope_hbm.at[b], rope_buf.at[ring, g], in_sem.at[ring, g, 1]))
        return out

    def writes(step):
        ring = lax.rem(step, RING)
        out = []
        for g in range(GROUP):
            b = order_ref[first + step * GROUP + g]
            out.append(pltpu.make_async_copy(lat_buf.at[ring, g], lat_out.at[b], out_sem.at[ring, g, 0]))
            out.append(pltpu.make_async_copy(rope_buf.at[ring, g], rope_out.at[b], out_sem.at[ring, g, 1]))
        return out

    @pl.when(t == 0)
    def _():
        for s in range(min(AHEAD, steps)):
            for c in reads(s):
                c.start()

    @pl.when(t >= RING - AHEAD)
    def _():
        for c in writes(t - (RING - AHEAD)):
            c.wait()

    @pl.when(t + AHEAD < steps)
    def _():
        for c in reads(t + AHEAD):
            c.start()

    for c in reads(t):
        c.wait()

    ring = lax.rem(t, RING)
    rows16 = lax.broadcasted_iota(jnp.int32, (16, 1), 0)
    lanes = lax.broadcasted_iota(jnp.int32, (1, 128), 1)
    rdim = ropen_ref.shape[1]
    eye = lax.broadcasted_iota(jnp.int32, (rdim, rdim), 0) == lax.broadcasted_iota(jnp.int32, (rdim, rdim), 1)
    for g in range(GROUP):
        i = first + t * GROUP + g
        s = pos_ref[i] - start
        inside = jnp.logical_and(s >= 0, s < slots)
        sc = jnp.where(inside, s, 0)
        r0 = pl.multiple_of((sc // 16) * 16, 16)
        hit = rows16 == jnp.where(inside, sc - r0, -1)
        blk = lat_buf[ring, g, pl.ds(r0, 16), :]
        new = latn_ref[pl.ds(i, 1), :]
        lat_buf[ring, g, pl.ds(r0, 16), :] = jnp.where(hit, new, blk.astype(jnp.float32)).astype(jnp.bfloat16)
        c0 = pl.multiple_of((sc // 128) * 128, 128)
        hitc = lanes == jnp.where(inside, sc - c0, -1)
        row = ropen_ref[pl.ds(i, 1), :]
        col = jnp.sum(jnp.where(eye, row, 0.0), axis=1, keepdims=True)
        rblk = rope_buf[ring, g, :, pl.ds(c0, 128)]
        rope_buf[ring, g, :, pl.ds(c0, 128)] = jnp.where(hitc, col, rblk.astype(jnp.float32)).astype(jnp.bfloat16)

    slot_ids = lax.broadcasted_iota(jnp.int32, (1, slots), 1) + start
    o0 = pl.multiple_of(own * half, half)
    o1 = pl.multiple_of((1 - own) * half, half)
    scores = []
    for g in range(GROUP):
        i = first + t * GROUP + g
        qa = jnp.concatenate([qa_ref[g, pl.ds(o0, half), :], qa_ref[g, pl.ds(o1, half), :]], axis=0)
        qr = jnp.concatenate([qr_ref[g, pl.ds(o0, half), :], qr_ref[g, pl.ds(o1, half), :]], axis=0)
        s = lax.dot_general(qa, lat_buf[ring, g], (((1,), (1,)), ((), ())), preferred_element_type=jnp.float32)
        s = (s + jnp.dot(qr, rope_buf[ring, g], preferred_element_type=jnp.float32)) * scale
        scores.append(jnp.where(slot_ids <= pos_ref[i], s, MASK_VALUE))
    ms = m_ref[...]
    ls = l_ref[...]
    for g in range(GROUP):
        i = first + t * GROUP + g
        m = jnp.max(scores[g], axis=1, keepdims=True)
        p = jnp.where(slot_ids <= pos_ref[i], jnp.exp(scores[g] - m), 0.0)
        l = jnp.sum(p, axis=1, keepdims=True)
        u = jnp.dot(p.astype(jnp.bfloat16), lat_buf[ring, g], preferred_element_type=jnp.float32)
        uo_ref[g] = u[:half]
        us_ref[g] = u[half:]
        j = t * GROUP + g
        ms = jnp.where(lanes == j, m, ms)
        ls = jnp.where(lanes == j, l, ls)
    m_ref[...] = ms
    l_ref[...] = ls

    for c in writes(t):
        c.start()

    @pl.when(t == steps - 1)
    def _():
        for s in range(max(0, steps - (RING - AHEAD)), steps):
            for c in writes(s):
                c.wait()


def attend_chunk(first, count, scale, order, pos, where, qa, qr, latn, ropen, lat, rope, prev):
    steps = count // GROUP
    heads, rank = qa.shape[1], qa.shape[2]
    rdim = qr.shape[2]
    slots = lat.shape[1]
    half = heads // 2
    base = first // GROUP
    any_spec = pl.BlockSpec(memory_space=pl.ANY)
    in_specs = [
        pl.BlockSpec((GROUP, heads, rank), lambda t, *_: (base + t, 0, 0)),
        pl.BlockSpec((GROUP, heads, rdim), lambda t, *_: (base + t, 0, 0)),
        pl.BlockSpec(latn.shape, lambda t, *_: (0, 0)),
        pl.BlockSpec(ropen.shape, lambda t, *_: (0, 0)),
        any_spec, any_spec,
    ]
    args = [order, pos, where, qa, qr, latn, ropen, lat, rope]
    aliases = {}
    if prev is not None:
        in_specs += [any_spec, any_spec]
        args += list(prev)
        aliases = {9: 4, 10: 5}
    return pl.pallas_call(
        functools.partial(attend_kernel, first, steps, scale),
        grid_spec=pltpu.PrefetchScalarGridSpec(
            num_scalar_prefetch=3,
            grid=(steps,),
            in_specs=in_specs,
            out_specs=[
                pl.BlockSpec((GROUP, half, rank), lambda t, *_: (t, 0, 0)),
                pl.BlockSpec((GROUP, half, rank), lambda t, *_: (t, 0, 0)),
                pl.BlockSpec((heads, 128), lambda t, *_: (0, 0)),
                pl.BlockSpec((heads, 128), lambda t, *_: (0, 0)),
                any_spec, any_spec,
            ],
            scratch_shapes=[
                pltpu.VMEM((RING, GROUP, slots, rank), jnp.bfloat16),
                pltpu.VMEM((RING, GROUP, rdim, slots), jnp.bfloat16),
                pltpu.SemaphoreType.DMA((RING, GROUP, 2)),
                pltpu.SemaphoreType.DMA((RING, GROUP, 2)),
            ],
        ),
        out_shape=[
            jax.ShapeDtypeStruct((count, half, rank), jnp.float32),
            jax.ShapeDtypeStruct((count, half, rank), jnp.float32),
            jax.ShapeDtypeStruct((heads, 128), jnp.float32),
            jax.ShapeDtypeStruct((heads, 128), jnp.float32),
            jax.ShapeDtypeStruct(lat.shape, jnp.bfloat16),
            jax.ShapeDtypeStruct(rope.shape, jnp.bfloat16),
        ],
        input_output_aliases=aliases,
        compiler_params=pltpu.CompilerParams(dimension_semantics=('arbitrary',), vmem_limit_bytes=56 * 2 ** 20),
        cost_estimate=pl.CostEstimate(
            flops=4 * count * heads * slots * rank * 16, bytes_accessed=count * slots * (rank + rdim) * 4, transcendentals=0),
        name='attend_chunk_%d' % first,
    )(*args)


def finish_kernel(place_ref, og_ref, o2_ref, hid_ref, w_hbm, out_ref, wbuf, part, got_c, sum_c, got_t, full, staged, o_got, w_sem, o_sem, c_sem, t_sem, ay_sem, ax_sem, af_sem, ac_sem):
    blocks, rows, width = part.shape
    half_blocks = blocks // 2
    r2, r4 = rows // 2, rows // 4
    depth = wbuf.shape[1]
    sp = lax.axis_index('sp')
    tp = lax.axis_index('tp')
    core = lax.rem(sp, 2)
    xpos = sp // 2
    sib = {'sp': sp + 1 - 2 * core}
    nbx = {'sp': lax.rem(sp + 2, 4)}
    nby = {'tp': 1 - tp}
    mesh_id = pl.DeviceIdType.MESH

    def remote(src, dst, sems, k, j, to):
        return pltpu.make_async_remote_copy(src_ref=src, dst_ref=dst, send_sem=sems.at[0, k, j], recv_sem=sems.at[1, k, j], device_id=to, device_id_type=mesh_id)

    def wcopy(j):
        col = lax.rem(j, half_blocks)
        return pltpu.make_async_copy(
            w_hbm.at[pl.ds(pl.multiple_of(core * depth, depth), depth), pl.ds(pl.multiple_of(col * width, width), width)],
            wbuf.at[lax.rem(j, wbuf.shape[0])], w_sem.at[lax.rem(j, wbuf.shape[0])])

    def spot(j, x, c, t):
        first = pl.multiple_of((j // half_blocks) * 4 * rows // 2 + ((x * 2 + c) * 2 + t) * r4, r4)
        return full.at[lax.rem(j, half_blocks), pl.ds(first, r4)]

    def send_o():
        return remote(o2_ref.at[pl.ds(rows, rows)], o_got, o_sem, 0, 0, nbx)

    def copy_c(j):
        return remote(part.at[j, pl.ds(pl.multiple_of((1 - core) * r2, r2), r2)], got_c.at[j], c_sem, 0, j, sib)

    def copy_t(j):
        return remote(sum_c.at[j, pl.ds(pl.multiple_of((1 - tp) * r4, r4), r4)], got_t.at[j], t_sem, 0, j, nby)

    def copy_ay(j):
        return remote(spot(j, xpos, core, tp), spot(j, xpos, core, tp), ay_sem, 0, j, nby)

    def copy_ax(j):
        return remote(spot(j, xpos, core, tp), spot(j, xpos, core, tp), ax_sem, 0, j, nbx)

    def copy_af(j):
        return remote(spot(j, xpos, core, 1 - tp), spot(j, xpos, core, 1 - tp), af_sem, 0, j, nbx)

    def copy_ac(j, k):
        x = xpos if k < 2 else 1 - xpos
        t = tp if k % 2 == 0 else 1 - tp
        return remote(spot(j, x, core, t), spot(j, x, core, t), ac_sem, k, j, sib)

    for j in range(wbuf.shape[0] - 1):
        wcopy(j).start()
    barrier = pltpu.get_barrier_semaphore()
    for to in (sib, nbx, nby):
        pl.semaphore_signal(barrier, inc=1, device_id=to, device_id_type=mesh_id)
    pl.semaphore_wait(barrier, 3)

    @pl.when(xpos == 0)
    def _():
        send_o().start()

    def body(i, carry):
        j = i

        @pl.when(j < blocks)
        def _():
            @pl.when(jnp.logical_and(j == half_blocks, xpos == 1))
            def _():
                send_o().wait_recv()

            wcopy(j).wait()
            w = wbuf.at[lax.rem(j, wbuf.shape[0])]

            @pl.when(j < half_blocks)
            def _():
                part[j] = jnp.dot(og_ref[...].astype(jnp.bfloat16), w[...], preferred_element_type=jnp.float32)

            @pl.when(j >= half_blocks)
            def _():
                o = jnp.where(xpos == 0, o2_ref[pl.ds(0, rows)], o_got[...])
                part[j] = jnp.dot(o.astype(jnp.bfloat16), w[...], preferred_element_type=jnp.float32)

            @pl.when(j + wbuf.shape[0] - 1 < blocks)
            def _():
                wcopy(j + wbuf.shape[0] - 1).start()

            copy_c(j).start()

        j1 = i - 1

        @pl.when(jnp.logical_and(j1 >= 0, j1 < blocks))
        def _():
            copy_c(j1).wait_recv()
            sum_c[j1] = part[j1, pl.ds(pl.multiple_of(core * r2, r2), r2)] + got_c[j1]
            copy_t(j1).start()

        j2 = i - 3

        @pl.when(jnp.logical_and(j2 >= 0, j2 < blocks))
        def _():
            copy_t(j2).wait_recv()
            first = pl.multiple_of((j2 // half_blocks) * 2 * rows + ((xpos * 2 + core) * 2 + tp) * r4, r4)
            full[lax.rem(j2, half_blocks), pl.ds(first, r4)] = sum_c[j2, pl.ds(pl.multiple_of(tp * r4, r4), r4)] + got_t[j2]
            copy_ay(j2).start()
            copy_ax(j2).start()
            copy_ac(j2, 0).start()

        j3 = i - 5

        @pl.when(jnp.logical_and(j3 >= 0, j3 < blocks))
        def _():
            copy_ay(j3).wait_recv()
            copy_af(j3).start()
            copy_ac(j3, 1).start()
            copy_ax(j3).wait_recv()
            copy_ac(j3, 2).start()

        j4 = i - 7

        @pl.when(jnp.logical_and(j4 >= 0, j4 < blocks))
        def _():
            copy_af(j4).wait_recv()
            copy_ac(j4, 3).start()

        j5 = i - 8

        @pl.when(jnp.logical_and(j5 >= 0, j5 < blocks))
        def _():
            for k in range(4):
                copy_ac(j5, k).wait_recv()

        @pl.when(jnp.logical_and(j5 >= half_blocks, j5 < blocks))
        def _():
            cb = j5 - half_blocks
            cols = pl.ds(pl.multiple_of(cb * width, width), width)
            staged[...] = full[cb]

            def emit(q, carry):
                b = pl.multiple_of(q * 16, 16)
                lines = [staged[pl.ds(place_ref[b + r], 1), :] for r in range(16)]
                y = jnp.concatenate(lines, axis=0)
                out_ref[pl.ds(b, 16), cols] = (hid_ref[pl.ds(b, 16), cols].astype(jnp.float32) + y).astype(jnp.bfloat16)
                return carry

            lax.fori_loop(0, out_ref.shape[0] // 16, emit, 0)

        return carry

    lax.fori_loop(0, blocks + 8, body, 0)

    def drain(j, carry):
        copy_c(j).wait_send()
        copy_t(j).wait_send()
        copy_ay(j).wait_send()
        copy_ax(j).wait_send()
        copy_af(j).wait_send()
        for k in range(4):
            copy_ac(j, k).wait_send()
        return carry

    lax.fori_loop(0, blocks, drain, 0)

    @pl.when(xpos == 0)
    def _():
        send_o().wait_send()


def finish(place, og, o2, hidden, w_out, blocks):
    rows, depth = og.shape
    batch, dmodel = hidden.shape
    width = dmodel // (blocks // 2)
    vmem = pl.BlockSpec(memory_space=pltpu.VMEM)
    ring = 4
    return pl.pallas_call(
        finish_kernel,
        in_specs=[pl.BlockSpec(memory_space=pltpu.SMEM), vmem, vmem, vmem, pl.BlockSpec(memory_space=pl.ANY)],
        out_specs=vmem,
        out_shape=jax.ShapeDtypeStruct((batch, dmodel), jnp.bfloat16),
        scratch_shapes=[
            pltpu.VMEM((ring, depth, width), jnp.bfloat16),
            pltpu.VMEM((blocks, rows, width), jnp.float32),
            pltpu.VMEM((blocks, rows // 2, width), jnp.float32),
            pltpu.VMEM((blocks, rows // 2, width), jnp.float32),
            pltpu.VMEM((blocks, rows // 4, width), jnp.float32),
            pltpu.VMEM((blocks // 2, batch, width), jnp.float32),
            pltpu.VMEM((batch, width), jnp.float32),
            pltpu.VMEM((rows, depth), jnp.float32),
            pltpu.SemaphoreType.DMA((ring,)),
            pltpu.SemaphoreType.DMA((2, 1, 1)),
            pltpu.SemaphoreType.DMA((2, 1, blocks)),
            pltpu.SemaphoreType.DMA((2, 1, blocks)),
            pltpu.SemaphoreType.DMA((2, 1, blocks)),
            pltpu.SemaphoreType.DMA((2, 1, blocks)),
            pltpu.SemaphoreType.DMA((2, 1, blocks)),
            pltpu.SemaphoreType.DMA((2, 4, blocks)),
        ],
        compiler_params=pltpu.CompilerParams(collective_id=1, has_side_effects=True, vmem_limit_bytes=60 * 2 ** 20),
        name='finish',
    )(place, og, o2, hidden, w_out)


def pair_kernel(m0_ref, l0_ref, m1_ref, l1_ref, uo_hbm, us_hbm, u_ref, m_ref, l_ref, got, own, mg, lg, ml_sem, d_sem, o_sem):
    blocks, rows = own.shape[0], own.shape[1]
    heads = own.shape[2]
    sp = lax.axis_index('sp')
    sib = {'sp': sp + 1 - 2 * lax.rem(sp, 2)}
    mesh_id = pl.DeviceIdType.MESH

    def remote(src, dst, sems, j):
        return pltpu.make_async_remote_copy(src_ref=src, dst_ref=dst, send_sem=sems.at[0, j], recv_sem=sems.at[1, j], device_id=sib, device_id_type=mesh_id)

    def mine(j):
        return pltpu.make_async_copy(uo_hbm.at[pl.ds(j * rows, rows)], own.at[j], o_sem.at[j])

    def theirs(j):
        return remote(us_hbm.at[pl.ds(j * rows, rows)], got.at[j], d_sem, j)

    barrier = pltpu.get_barrier_semaphore()
    pl.semaphore_signal(barrier, inc=1, device_id=sib, device_id_type=mesh_id)
    for j in range(blocks):
        mine(j).start()
    pl.semaphore_wait(barrier, 1)
    cm = remote(m1_ref, mg, ml_sem, 0)
    cl = remote(l1_ref, lg, ml_sem, 1)
    cm.start()
    cl.start()
    for j in range(blocks):
        theirs(j).start()
    cm.wait()
    cl.wait()
    m0, m1 = m0_ref[...], mg[...]
    m = jnp.maximum(m0, m1)
    a0 = jnp.exp(m0 - m)
    a1 = jnp.exp(m1 - m)
    m_ref[...] = m
    l_ref[...] = l0_ref[...] * a0 + lg[...] * a1
    lanes = lax.broadcasted_iota(jnp.int32, (1, 128), 1)

    def body(j, carry):
        mine(j).wait()
        theirs(j).wait_recv()
        for r in range(rows):
            hit = lanes == j * rows + r
            c0 = jnp.sum(jnp.where(hit, a0, 0.0), axis=1, keepdims=True)
            c1 = jnp.sum(jnp.where(hit, a1, 0.0), axis=1, keepdims=True)
            u_ref[j * rows + r] = own[j, r] * c0 + got[j, r] * c1
        return carry

    lax.fori_loop(0, blocks, body, 0)

    def drain(j, carry):
        theirs(j).wait_send()
        return carry

    lax.fori_loop(0, blocks, drain, 0)


def pair_merge(m, l, uo, us, tag):
    count, half, rank = uo.shape
    rows = 8
    blocks = count // rows
    vmem = pl.BlockSpec(memory_space=pltpu.VMEM)
    any_spec = pl.BlockSpec(memory_space=pl.ANY)
    return pl.pallas_call(
        pair_kernel,
        in_specs=[vmem, vmem, vmem, vmem, any_spec, any_spec],
        out_specs=[vmem, vmem, vmem],
        out_shape=[
            jax.ShapeDtypeStruct((count, half, rank), jnp.float32),
            jax.ShapeDtypeStruct((half, 128), jnp.float32),
            jax.ShapeDtypeStruct((half, 128), jnp.float32),
        ],
        scratch_shapes=[
            pltpu.VMEM((blocks, rows, half, rank), jnp.float32),
            pltpu.VMEM((blocks, rows, half, rank), jnp.float32),
            pltpu.VMEM((half, 128), jnp.float32),
            pltpu.VMEM((half, 128), jnp.float32),
            pltpu.SemaphoreType.DMA((2, 2)),
            pltpu.SemaphoreType.DMA((2, blocks)),
            pltpu.SemaphoreType.DMA((blocks,)),
        ],
        compiler_params=pltpu.CompilerParams(collective_id=tag, has_side_effects=True, vmem_limit_bytes=60 * 2 ** 20),
        name='pair_merge_%d' % tag,
    )(m[:half], l[:half], m[half:], l[half:], uo, us)


def merge(m0, l0, u0, m1, l1, u1):
    m = jnp.maximum(m0, m1)
    a0 = jnp.exp(m0 - m)
    a1 = jnp.exp(m1 - m)
    return m, l0 * a0 + l1 * a1, u0 * a0[:, :, None] + u1 * a1[:, :, None]


def solution(mesh):
    row_spec = P('dp', None)
    cache_spec = P('dp', 'sp', None)
    head_spec = P(None, 'tp', None)
    in_specs = (row_spec, cache_spec, cache_spec, P('dp'), P(), P(), P(), P(), head_spec, head_spec, head_spec, P('tp', None))
    out_specs = (row_spec, cache_spec, cache_spec)
    sibling = [(0, 1), (1, 0), (2, 3), (3, 2)]
    across = [(0, 2), (2, 0), (1, 3), (3, 1)]

    def local_step(hidden, lat_cache, rope_cache, positions, w_dq, gain_q, w_dkv, gain_kv, w_uq, w_uk, w_uv, w_out):
        rows = hidden.shape[0]
        slots = lat_cache.shape[1]
        heads = w_uq.shape[1]
        half = heads // 2
        scale = YARN_MSCALE ** 2 / math.sqrt(w_uq.shape[2])
        sp = lax.axis_index('sp')
        core = sp % 2
        xpos = sp // 2
        ids = jnp.arange(rows, dtype=jnp.int32)
        ahead = (positions[None, :] > positions[:, None]) | ((positions[None, :] == positions[:, None]) & (ids[None, :] < ids[:, None]))
        rank_of = jnp.sum(ahead.astype(jnp.int32), axis=1)
        pick = rank_of[None, :] == ids[:, None]
        order = jnp.sum(jnp.where(pick, ids[None, :], 0), axis=1)
        pos = jnp.sum(jnp.where(pick, positions[None, :], 0), axis=1)
        hid = jnp.dot((order[:, None] == ids[None, :]).astype(jnp.bfloat16), hidden, preferred_element_type=jnp.float32).astype(jnp.bfloat16)
        q_abs, q_rope, lat_new, rope_new = project_inputs(hid, pos, w_dq, gain_q, w_dkv, gain_kv, w_uq, w_uk)
        latn = lat_new.astype(jnp.float32)
        ropen = rope_new.astype(jnp.float32)
        rope_t = jnp.swapaxes(rope_cache, 1, 2)
        where = jnp.stack([sp * slots, core]).astype(jnp.int32)

        half_rows = rows // 2
        own_rows = rows // 4
        prev = None
        parts = []
        for g in range(2):
            if g == 1:
                tied = lax.optimization_barrier((where, keep, send))
                where, keep, send = tied
            uo, us, m, l, lo, ro = attend_chunk(g * half_rows, half_rows, scale, order, pos, where, q_abs, q_rope, latn, ropen, lat_cache, rope_t, prev)
            prev = (lo, ro)
            u, m, l = pair_merge(m, l, uo, us, 2 + g)
            m, l = m[:, :half_rows].T, l[:, :half_rows].T
            if g == 0:
                keep = [lax.dynamic_slice_in_dim(v, xpos * own_rows, own_rows, 0) for v in (m, l, u)]
                send = [lax.dynamic_slice_in_dim(v, (1 - xpos) * own_rows, own_rows, 0) for v in (m, l, u)]
        got = lax.ppermute(send, 'sp', across)
        _, l1, u1 = merge(*keep, *got)
        lat1 = (u1 / l1[:, :, None]).astype(jnp.bfloat16)
        lat_out, rope_out = prev[0], jnp.swapaxes(prev[1], 1, 2)

        def near(args):
            _, l, u = args
            return (u / jnp.where(l > 0, l, 1.0)[:, :, None]).astype(jnp.bfloat16)

        def far(args):
            got = lax.ppermute(list(args), 'sp', across)
            return near(merge(*args, *got))

        lat2 = lax.cond(pos[half_rows] >= 2 * slots, far, near, (m, l, u))
        w_uv_own = lax.dynamic_slice_in_dim(w_uv, core * half, half, 1)
        og = jnp.einsum('bhk,khv->bhv', lat1, w_uv_own, preferred_element_type=jnp.float32).reshape(own_rows, -1)
        o2 = jnp.einsum('bhk,khv->bhv', lat2, w_uv_own, preferred_element_type=jnp.float32).reshape(half_rows, -1)
        r = rank_of % half_rows
        x, k = r // own_rows, r % own_rows
        quarter = own_rows // 4
        c, t = k // (2 * quarter), (k // quarter) % 2
        place = (rank_of // half_rows) * half_rows + ((x * 2 + c) * 2 + t) * quarter + k % quarter
        out = finish(place.astype(jnp.int32), og, o2, hidden, w_out, 12)
        return out, lat_out, rope_out

    return jax.shard_map(local_step, mesh=mesh, in_specs=in_specs, out_specs=out_specs, check_vma=False)
```

```python
import functools
import math
import jax
import jax.numpy as jnp
from jax import lax
from jax.experimental import pallas as pl
from jax.experimental.pallas import tpu as pltpu
from jax.sharding import PartitionSpec as P

EPSILON = 1e-6
ROPE_BASE = 50000.0
YARN_MSCALE = 1.0 + 0.1 * math.log(32.0)
MASK_VALUE = -1e30
GROUP = 8
RING = 4
AHEAD = 2
VIA_Y = 0
LANES = 128
PACK = 16
VMEM_BYTES = 67043328
VMEM_STEP = 1048576


def rope_tables(positions, rope_dim):
    half_dim = rope_dim // 2
    inv_freq = ROPE_BASE ** (-jnp.arange(half_dim).astype(jnp.float32) / half_dim)
    angles = positions.astype(jnp.float32)[:, None] * inv_freq[None, :]
    return jnp.cos(angles), jnp.sin(angles)


def insert_slot(i, start, pos_ref, latn_ref, ropen_ref, lat, rope):
    slots = lat.shape[0]
    rdim = rope.shape[0]
    s = pos_ref[i] - start
    inside = jnp.logical_and(s >= 0, s < slots)
    sc = jnp.where(inside, s, 0)
    r0 = pl.multiple_of((sc // PACK) * PACK, PACK)
    hit = lax.broadcasted_iota(jnp.int32, (PACK, 1), 0) == jnp.where(inside, sc - r0, -1)
    blk = lat[pl.ds(r0, PACK), :]
    lat[pl.ds(r0, PACK), :] = jnp.where(hit, latn_ref[pl.ds(i, 1), :], blk.astype(jnp.float32)).astype(jnp.bfloat16)
    c0 = pl.multiple_of((sc // LANES) * LANES, LANES)
    hit = lax.broadcasted_iota(jnp.int32, (1, LANES), 1) == jnp.where(inside, sc - c0, -1)
    eye = lax.broadcasted_iota(jnp.int32, (rdim, rdim), 0) == lax.broadcasted_iota(jnp.int32, (rdim, rdim), 1)
    col = jnp.sum(jnp.where(eye, ropen_ref[pl.ds(i, 1), :], 0.0), axis=1, keepdims=True)
    blk = rope[:, pl.ds(c0, LANES)]
    rope[:, pl.ds(c0, LANES)] = jnp.where(hit, col, blk.astype(jnp.float32)).astype(jnp.bfloat16)


def heads_kernel(cq_ref, cos_ref, sin_ref, wuq_ref, wuk_ref, qa_ref, qr_ref, wide, lines, rlines):
    block = wuq_ref.shape[0]
    nope = wuk_ref.shape[2]
    rank = wuk_ref.shape[0]
    rdim = wuq_ref.shape[1] - nope
    hdim = rdim // 2
    wide[...] = wuk_ref[...].astype(jnp.float32)
    cq = cq_ref[...]
    depth = cq.shape[1]
    dims = (((1,), (1,)), ((), ()))
    w_rope = wuq_ref[:, nope:, :].reshape(block * rdim, depth)
    r = lax.dot_general(cq, w_rope, dims, preferred_element_type=jnp.float32).astype(jnp.bfloat16).astype(jnp.float32)
    lane = lax.broadcasted_iota(jnp.int32, (1, block * rdim), 1)
    width = block * rdim
    turned = jnp.where(lane % rdim < hdim, -pltpu.roll(r, width - hdim, 1), pltpu.roll(r, hdim, 1))
    r = r * jnp.concatenate([cos_ref[...]] * block, axis=1) + turned * jnp.concatenate([sin_ref[...]] * block, axis=1)
    w_nope = wuq_ref[:, :nope, :].reshape(block * nope, depth)
    q = lax.dot_general(cq, w_nope, dims, preferred_element_type=jnp.float32).astype(jnp.bfloat16)
    for h in range(block):
        rlines[:, h, :rdim] = r[:, h * rdim:(h + 1) * rdim]
        wk = wide[:, h, :].astype(jnp.bfloat16)
        lines[:, h, :rank] = lax.dot_general(q[:, h * nope:(h + 1) * nope], wk, dims, preferred_element_type=jnp.float32)
    qa_ref[...] = lines[:, :, :rank].astype(jnp.bfloat16)
    qr_ref[...] = rlines[:, :, :rdim].astype(jnp.bfloat16)


def head_queries(cq, cos2, sin2, w_uq_t, w_uk):
    rows, qrank = cq.shape
    heads, qdim, _ = w_uq_t.shape
    rank, _, nope = w_uk.shape
    rdim = qdim - nope
    block = GROUP
    f32 = jnp.float32
    whole = lambda v: pl.BlockSpec(v.shape, lambda i: (0, 0))
    return pl.pallas_call(
        heads_kernel,
        grid=(heads // block,),
        in_specs=[
            whole(cq), whole(cos2), whole(sin2),
            pl.BlockSpec((block, qdim, qrank), lambda i: (i, 0, 0)),
            pl.BlockSpec((rank, block, nope), lambda i: (0, i, 0)),
        ],
        out_specs=[pl.BlockSpec((rows, block, d), lambda i: (0, i, 0)) for d in (rank, rdim)],
        out_shape=[jax.ShapeDtypeStruct((rows, heads, d), jnp.bfloat16) for d in (rank, rdim)],
        scratch_shapes=[
            pltpu.VMEM((rank, block, nope), f32),
            pltpu.VMEM((rows, block, rank + LANES), f32),
            pltpu.VMEM((rows, block, LANES), f32),
        ],
        compiler_params=pltpu.CompilerParams(dimension_semantics=('arbitrary',), vmem_limit_bytes=VMEM_BYTES - 8 * VMEM_STEP),
        cost_estimate=pl.CostEstimate(flops=2 * rows * heads * (qdim * qrank + nope * rank), bytes_accessed=2 * heads * (qdim * qrank + nope * rank), transcendentals=0),
        name='head_queries',
    )(cq, cos2, sin2, w_uq_t, w_uk)


def down_kernel(order_ref, hid_ref, wdq_ref, wkv_ref, gq_ref, gkv_ref, cos_ref, sin_ref, cq_ref, latn_ref, ropen_ref, pick, acc_q, acc_kv):
    i = pl.program_id(0)
    rows = hid_ref.shape[0]
    rank = gkv_ref.shape[0]
    hdim = cos_ref.shape[1] // 2

    @pl.when(i == 0)
    def _():
        pick[...] = (order_ref[...] == lax.broadcasted_iota(jnp.int32, (rows, rows), 1)).astype(jnp.bfloat16)
        acc_q[...] = jnp.zeros_like(acc_q)
        acc_kv[...] = jnp.zeros_like(acc_kv)

    x = jnp.dot(pick[...], hid_ref[...], preferred_element_type=jnp.float32).astype(jnp.bfloat16)
    acc_q[...] += jnp.dot(x, wdq_ref[...], preferred_element_type=jnp.float32)
    acc_kv[...] += lax.dot_general(x, wkv_ref[...], (((1,), (1,)), ((), ())), preferred_element_type=jnp.float32)

    @pl.when(i == pl.num_programs(0) - 1)
    def _():
        def normed(v, gain):
            v = v.astype(jnp.bfloat16).astype(jnp.float32)
            inv = lax.rsqrt(jnp.mean(v * v, axis=-1, keepdims=True) + EPSILON)
            return (v * inv * gain.astype(jnp.float32)[None, :]).astype(jnp.bfloat16)

        cq_ref[...] = normed(acc_q[...], gq_ref[...])
        latn_ref[...] = normed(acc_kv[:, :rank], gkv_ref[...]).astype(jnp.float32)
        r = acc_kv[:, rank:].astype(jnp.bfloat16).astype(jnp.float32)
        turned = jnp.concatenate([-r[:, hdim:], r[:, :hdim]], axis=1)
        ropen_ref[...] = (r * cos_ref[...] + turned * sin_ref[...]).astype(jnp.bfloat16).astype(jnp.float32)


def down_project(order, hidden, w_dq, w_dkv_t, gain_q, gain_kv, cos2, sin2):
    rows, dmodel = hidden.shape
    qrank = w_dq.shape[1]
    width = w_dkv_t.shape[0]
    rank = gain_kv.shape[0]
    block = 1024
    fixed = lambda i: (0, 0)
    return pl.pallas_call(
        down_kernel,
        grid=(dmodel // block,),
        in_specs=[
            pl.BlockSpec((rows, 1), fixed),
            pl.BlockSpec((rows, block), lambda i: (0, i)),
            pl.BlockSpec((block, qrank), lambda i: (i, 0)),
            pl.BlockSpec((width, block), lambda i: (0, i)),
            pl.BlockSpec((qrank,), lambda i: (0,)),
            pl.BlockSpec((rank,), lambda i: (0,)),
            pl.BlockSpec(cos2.shape, fixed),
            pl.BlockSpec(sin2.shape, fixed),
        ],
        out_specs=[pl.BlockSpec((rows, qrank), fixed), pl.BlockSpec((rows, rank), fixed), pl.BlockSpec((rows, width - rank), fixed)],
        out_shape=[
            jax.ShapeDtypeStruct((rows, qrank), jnp.bfloat16),
            jax.ShapeDtypeStruct((rows, rank), jnp.float32),
            jax.ShapeDtypeStruct((rows, width - rank), jnp.float32),
        ],
        scratch_shapes=[
            pltpu.VMEM((rows, rows), jnp.bfloat16),
            pltpu.VMEM((rows, qrank), jnp.float32),
            pltpu.VMEM((rows, width), jnp.float32),
        ],
        compiler_params=pltpu.CompilerParams(dimension_semantics=('arbitrary',), vmem_limit_bytes=VMEM_BYTES - 8 * VMEM_STEP),
        cost_estimate=pl.CostEstimate(flops=2 * rows * dmodel * (qrank + width + rows), bytes_accessed=2 * dmodel * (qrank + width), transcendentals=0),
        name='down_project',
    )(order[:, None], hidden, w_dq, w_dkv_t, gain_q, gain_kv, cos2, sin2)


def attend_kernel(first, steps, scale, order_ref, pos_ref, where_ref, qa_ref, qr_ref, latn_ref, ropen_ref, lat_hbm, rope_hbm, *rest):
    uo_ref, us_ref, mo_ref, lo_ref, ms_ref, ls_ref, lat_out, rope_out, lat_buf, rope_buf, in_sem, out_sem = rest[-12:]
    t = pl.program_id(0)
    slots = lat_buf.shape[2]
    heads = qa_ref.shape[1]
    half = heads // 2
    start = where_ref[0]
    own = where_ref[1]

    def reads(step):
        ring = lax.rem(step, RING)
        out = []
        for g in range(GROUP):
            b = order_ref[first + step * GROUP + g]
            out.append(pltpu.make_async_copy(lat_hbm.at[b], lat_buf.at[ring, g], in_sem.at[ring, g, 0]))
            out.append(pltpu.make_async_copy(rope_hbm.at[b], rope_buf.at[ring, g], in_sem.at[ring, g, 1]))
        return out

    def writes(step):
        ring = lax.rem(step, RING)
        out = []
        for g in range(GROUP):
            b = order_ref[first + step * GROUP + g]
            out.append(pltpu.make_async_copy(lat_buf.at[ring, g], lat_out.at[b], out_sem.at[ring, g, 0]))
            out.append(pltpu.make_async_copy(rope_buf.at[ring, g], rope_out.at[b], out_sem.at[ring, g, 1]))
        return out

    @pl.when(t == 0)
    def _():
        for s in range(min(AHEAD, steps)):
            for c in reads(s):
                c.start()

    lag = RING - AHEAD

    @pl.when(t >= lag)
    def _():
        for c in writes(t - lag):
            c.wait()

    @pl.when(t + AHEAD < steps)
    def _():
        for c in reads(t + AHEAD):
            c.start()

    for c in reads(t):
        c.wait()

    ring = lax.rem(t, RING)
    lanes = lax.broadcasted_iota(jnp.int32, (1, LANES), 1)
    for g in range(GROUP):
        insert_slot(first + t * GROUP + g, start, pos_ref, latn_ref, ropen_ref, lat_buf.at[ring, g], rope_buf.at[ring, g])

    slot_ids = lax.broadcasted_iota(jnp.int32, (1, slots), 1) + start
    o0 = pl.multiple_of(own * half, half)
    o1 = pl.multiple_of((1 - own) * half, half)
    scores = []
    for g in range(GROUP):
        i = first + t * GROUP + g
        qa = jnp.concatenate([qa_ref[g, pl.ds(o0, half), :], qa_ref[g, pl.ds(o1, half), :]], axis=0)
        qr = jnp.concatenate([qr_ref[g, pl.ds(o0, half), :], qr_ref[g, pl.ds(o1, half), :]], axis=0)
        s = lax.dot_general(qa, lat_buf[ring, g], (((1,), (1,)), ((), ())), preferred_element_type=jnp.float32)
        s = (s + jnp.dot(qr, rope_buf[ring, g], preferred_element_type=jnp.float32)) * scale
        scores.append(jnp.where(slot_ids <= pos_ref[i], s, MASK_VALUE))
    ms = jnp.concatenate([mo_ref[...], ms_ref[...]], axis=0)
    ls = jnp.concatenate([lo_ref[...], ls_ref[...]], axis=0)
    for g in range(GROUP):
        i = first + t * GROUP + g
        m = jnp.max(scores[g], axis=1, keepdims=True)
        p = jnp.where(slot_ids <= pos_ref[i], jnp.exp(scores[g] - m), 0.0)
        l = jnp.sum(p, axis=1, keepdims=True)
        u = jnp.dot(p.astype(jnp.bfloat16), lat_buf[ring, g], preferred_element_type=jnp.float32)
        uo_ref[g] = u[:half]
        us_ref[g] = u[half:]
        j = t * GROUP + g
        ms = jnp.where(lanes == j, m, ms)
        ls = jnp.where(lanes == j, l, ls)
    mo_ref[...] = ms[:half]
    lo_ref[...] = ls[:half]
    ms_ref[...] = ms[half:]
    ls_ref[...] = ls[half:]

    for c in writes(t):
        c.start()

    @pl.when(t == steps - 1)
    def _():
        for s in range(max(0, steps - lag), steps):
            for c in writes(s):
                c.wait()


def attend_chunk(first, count, scale, order, pos, where, qa, qr, latn, ropen, lat, rope, prev):
    steps = count // GROUP
    heads, rank = qa.shape[1:]
    rdim = qr.shape[2]
    slots = lat.shape[1]
    half = heads // 2
    base = first // GROUP
    any_spec = pl.BlockSpec(memory_space=pl.ANY)
    fixed = lambda t, *_: (0, 0)
    bf16, f32 = jnp.bfloat16, jnp.float32
    dma = pltpu.SemaphoreType.DMA((RING, GROUP, 2))
    part = jax.ShapeDtypeStruct((count, half, rank), f32)
    tile = jax.ShapeDtypeStruct((half, LANES), f32)
    return pl.pallas_call(
        functools.partial(attend_kernel, first, steps, scale),
        grid_spec=pltpu.PrefetchScalarGridSpec(
            num_scalar_prefetch=3,
            grid=(steps,),
            in_specs=[pl.BlockSpec((GROUP, heads, d), lambda t, *_: (base + t, 0, 0)) for d in (rank, rdim)]
            + [pl.BlockSpec(v.shape, fixed) for v in (latn, ropen)] + [any_spec] * (2 + len(prev)),
            out_specs=[pl.BlockSpec((GROUP, half, rank), lambda t, *_: (t, 0, 0))] * 2 + [pl.BlockSpec(tile.shape, fixed)] * 4 + [any_spec] * 2,
            scratch_shapes=[
                pltpu.VMEM((RING, GROUP, slots, rank), bf16),
                pltpu.VMEM((RING, GROUP, rdim, slots), bf16),
                dma, dma,
            ],
        ),
        out_shape=[part] * 2 + [tile] * 4 + [jax.ShapeDtypeStruct(v.shape, bf16) for v in (lat, rope)],
        input_output_aliases={9: 6, 10: 7} if prev else {},
        compiler_params=pltpu.CompilerParams(dimension_semantics=('arbitrary',), vmem_limit_bytes=VMEM_BYTES - 8 * VMEM_STEP),
        cost_estimate=pl.CostEstimate(
            flops=64 * count * heads * slots * rank, bytes_accessed=count * slots * (rank + rdim) * 4, transcendentals=0),
        name='attend_chunk_%d' % first,
    )(order, pos, where, qa, qr, latn, ropen, lat, rope, *prev)


def finish_kernel(place_ref, mk_ref, lk_ref, m0_ref, l0_ref, m1_ref, l1_ref, uk_hbm, ux_hbm, uo_hbm, us_hbm, wvh_hbm, hid_hbm, w_hbm, out_hbm, wbuf, part, got_c, sum_c, got_t, full, staged, o_got, o1, o2, ua, ux, ub, ud, un, wv_heads, mg, lg, hid, outv, w_sem, o_sem, c_sem, t_sem, ay_sem, ax_sem, af_sem, ac_sem, a_sem, b_sem, d_sem, ml_sem, v_sem, h_sem, r_sem):
    blocks, rows, width = part.shape
    half_blocks = blocks // 2
    r2, r4 = rows // 2, rows // 4
    depth = wbuf.shape[1]
    sp = lax.axis_index('sp')
    tp = lax.axis_index('tp')
    core = lax.rem(sp, 2)
    xpos = sp // 2
    sib = {'sp': sp + 1 - 2 * core}
    nbx = {'sp': lax.rem(sp + 2, 4)}
    nby = {'tp': 1 - tp}
    mesh_id = pl.DeviceIdType.MESH

    def remote(src, dst, sems, j, to, k=0):
        return pltpu.make_async_remote_copy(src_ref=src, dst_ref=dst, send_sem=sems.at[0, k, j], recv_sem=sems.at[1, k, j], device_id=to, device_id_type=mesh_id)

    def wcopy(j):
        col = lax.rem(j, half_blocks)
        return pltpu.make_async_copy(
            w_hbm.at[pl.ds(pl.multiple_of(core * depth, depth), depth), pl.ds(pl.multiple_of(col * width, width), width)],
            wbuf.at[lax.rem(j, wbuf.shape[0])], w_sem.at[lax.rem(j, wbuf.shape[0])])

    def spot(j, x, c, t):
        first = pl.multiple_of((j // half_blocks) * 4 * rows // 2 + ((x * 2 + c) * 2 + t) * r4, r4)
        return full.at[lax.rem(j, half_blocks), pl.ds(first, r4)]

    def send_o():
        return remote(o2.at[pl.ds(rows, rows)], o_got, o_sem, 0, nbx)

    def copy_c(j):
        return remote(part.at[j, pl.ds(pl.multiple_of((1 - core) * r2, r2), r2)], got_c.at[j], c_sem, j, sib)

    def copy_t(j):
        return remote(sum_c.at[j, pl.ds(pl.multiple_of((1 - tp) * r4, r4), r4)], got_t.at[j], t_sem, j, nby)

    def copy_ay(j):
        return remote(spot(j, xpos, core, tp), spot(j, xpos, core, tp), ay_sem, j, nby)

    def copy_ax(j):
        return remote(spot(j, xpos, core, tp), spot(j, xpos, core, tp), ax_sem, j, nbx)

    def copy_af(j):
        return remote(spot(j, xpos, core, 1 - tp), spot(j, xpos, core, 1 - tp), af_sem, j, nbx)

    def copy_ag(j):
        return remote(spot(j, 1 - xpos, core, tp), spot(j, 1 - xpos, core, tp), af_sem, j, nby)

    via_y = VIA_Y

    def emit_out(cb):
        cols = pl.ds(pl.multiple_of(cb * width, width), width)
        return pltpu.make_async_copy(outv.at[:, cols], out_hbm.at[:, cols], r_sem.at[cb])

    def copy_ac(j, k):
        x = xpos if k < 2 else 1 - xpos
        t = tp if k % 2 == 0 else 1 - tp
        return remote(spot(j, x, core, t), spot(j, x, core, t), ac_sem, j, sib, k)

    half = uk_hbm.shape[1]
    vdim = wvh_hbm.shape[2]
    quad = half // 2
    steps_b = ud.shape[0]
    rows_b = ud.shape[1]
    side_b = steps_b // 2

    def mine_a(k):
        if k == 0:
            return pltpu.make_async_copy(uk_hbm, ua, a_sem.at[0])
        return pltpu.make_async_copy(ux_hbm, ux, a_sem.at[1])

    def mine_b(k):
        return pltpu.make_async_copy(uo_hbm.at[pl.ds(k * rows_b, rows_b)], ub.at[k], b_sem.at[k])

    def theirs_b(k):
        return remote(us_hbm.at[pl.ds(k * rows_b, rows_b)], ud.at[k], d_sem, k, sib)

    get_wv = pltpu.make_async_copy(wvh_hbm, wv_heads, v_sem)
    get_hid = pltpu.make_async_copy(hid_hbm, hid, h_sem)
    order_b = list(range(side_b, steps_b)) + list(range(side_b))
    for k in range(2):
        mine_a(k).start()
    get_wv.start()
    for j in range(wbuf.shape[0] - 1):
        wcopy(j).start()
    for k in order_b:
        mine_b(k).start()
    get_hid.start()
    barrier = pltpu.get_barrier_semaphore()
    for to in (sib, nbx, nby):
        pl.semaphore_signal(barrier, inc=1, device_id=to, device_id_type=mesh_id)
    pl.semaphore_wait(barrier, 3)
    tiles = [remote(src, dst, ml_sem, k, sib) for k, (src, dst) in enumerate(((m1_ref, mg), (l1_ref, lg)))]
    for c in tiles:
        c.start()
    for k in order_b:
        theirs_b(k).start()

    lanes = lax.broadcasted_iota(jnp.int32, (1, 128), 1)

    def weights(m0, l0, m1, l1):
        m = jnp.maximum(m0, m1)
        a0 = jnp.exp(m0 - m)
        a1 = jnp.exp(m1 - m)
        l = l0 * a0 + l1 * a1
        inv = 1.0 / jnp.where(l > 0, l, 1.0)
        return a0 * inv, a1 * inv

    def merge_row(w, lane, first, second, to):
        hit = lanes == lane
        c0 = jnp.sum(jnp.where(hit, w[0], 0.0), axis=1, keepdims=True)
        c1 = jnp.sum(jnp.where(hit, w[1], 0.0), axis=1, keepdims=True)
        u = first * c0 + second * c1
        un[0, to, :, :u.shape[1]] = u[:quad]
        un[1, to, :, :u.shape[1]] = u[quad:]

    rank = uk_hbm.shape[2]

    def heads_out(to, first):
        def one(h, carry):
            for p in range(2):
                u = un[p, :, h, :rank].astype(jnp.bfloat16)
                o = jnp.dot(u, wv_heads[p * quad + h], preferred_element_type=jnp.float32)
                to[pl.ds(first, rows), pl.ds(pl.multiple_of((p * quad + h) * vdim, vdim), vdim)] = o.astype(to.dtype)
            return carry
        for h in range(quad):
            one(h, 0)

    def rows_of(k, q):
        mine_b(k).wait()
        theirs_b(k).wait_recv()
        w = weights(m0_ref[...], l0_ref[...], mg[...], lg[...])
        for e in range(rows_b):
            merge_row(w, k * rows_b + e, ub[k, e], ud[k, e], pl.multiple_of(q * rows_b, rows_b) + e)

    def first_side(q, carry):
        rows_of(side_b + q, q)
        return carry

    for k in range(2):
        mine_a(k).wait()
    wa = weights(mk_ref[...], lk_ref[...], ux[rows, :, :128], ux[rows, :, 128:256])

    def rows_a(q, carry):
        for e in range(8):
            r = q * 8 + e
            merge_row(wa, xpos * rows + r, ua[r], ux[r], r)
        return carry

    lax.fori_loop(0, rows // 8, rows_a, 0)
    get_wv.wait()
    heads_out(o1, 0)
    for c in tiles:
        c.wait()

    def second_group(i):
        per = side_b // 2

        @pl.when(i == 1)
        def _():
            lax.fori_loop(0, side_b, first_side, 0)
            heads_out(o2, rows)

            @pl.when(xpos == 0)
            def _():
                send_o().start()

        @pl.when(jnp.logical_and(i >= 3, i < 5))
        def _():
            def one(e, carry):
                q = (i - 3) * per + e
                rows_of(q, q)
                return carry

            lax.fori_loop(0, per, one, 0)

        @pl.when(i == 4)
        def _():
            heads_out(o2, 0)

    def body(i, carry):
        j = i

        @pl.when(j < blocks)
        def _():
            @pl.when(jnp.logical_and(j == half_blocks, xpos == 1))
            def _():
                send_o().wait_recv()

            wcopy(j).wait()
            w = wbuf.at[lax.rem(j, wbuf.shape[0])]

            @pl.when(j < half_blocks)
            def _():
                part[j] = jnp.dot(o1[...], w[...], preferred_element_type=jnp.float32)

            @pl.when(j >= half_blocks)
            def _():
                o = jnp.where(xpos == 0, o2[pl.ds(0, rows)], o_got[...])
                part[j] = jnp.dot(o.astype(jnp.bfloat16), w[...], preferred_element_type=jnp.float32)

            @pl.when(j + wbuf.shape[0] - 1 < blocks)
            def _():
                wcopy(j + wbuf.shape[0] - 1).start()

            copy_c(j).start()

        j1 = i - 1

        @pl.when(jnp.logical_and(j1 >= 0, j1 < blocks))
        def _():
            copy_c(j1).wait_recv()
            sum_c[j1] = part[j1, pl.ds(pl.multiple_of(core * r2, r2), r2)] + got_c[j1]
            copy_t(j1).start()

        second_group(i)

        j2 = i - 3

        @pl.when(jnp.logical_and(j2 >= 0, j2 < blocks))
        def _():
            copy_t(j2).wait_recv()
            first = pl.multiple_of((j2 // half_blocks) * 2 * rows + ((xpos * 2 + core) * 2 + tp) * r4, r4)
            full[lax.rem(j2, half_blocks), pl.ds(first, r4)] = sum_c[j2, pl.ds(pl.multiple_of(tp * r4, r4), r4)] + got_t[j2]
            copy_ay(j2).start()
            copy_ax(j2).start()
            copy_ac(j2, 0).start()

        j3 = i - 5

        @pl.when(jnp.logical_and(j3 >= 0, j3 < blocks))
        def _():
            copy_ay(j3).wait_recv()

            @pl.when(j3 >= via_y)
            def _():
                copy_af(j3).start()

            copy_ac(j3, 1).start()
            copy_ax(j3).wait_recv()

            @pl.when(j3 < via_y)
            def _():
                copy_ag(j3).start()

            copy_ac(j3, 2).start()

        j4 = i - 7

        @pl.when(jnp.logical_and(j4 >= 0, j4 < blocks))
        def _():
            copy_af(j4).wait_recv()
            copy_ac(j4, 3).start()

        j5 = i - 8

        @pl.when(jnp.logical_and(j5 >= 0, j5 < blocks))
        def _():
            for k in range(4):
                copy_ac(j5, k).wait_recv()

        @pl.when(jnp.logical_and(j5 >= half_blocks, j5 < blocks))
        def _():
            cb = j5 - half_blocks
            cols = pl.ds(pl.multiple_of(cb * width, width), width)
            staged[...] = full[cb]

            @pl.when(cb == 0)
            def _():
                get_hid.wait()


            def emit(q, carry):
                b = pl.multiple_of(q * 16, 16)
                lines = [staged[pl.ds(place_ref[b + r], 1), :] for r in range(16)]
                y = jnp.concatenate(lines, axis=0)
                outv[pl.ds(b, 16), cols] = (hid[pl.ds(b, 16), cols].astype(jnp.float32) + y).astype(jnp.bfloat16)
                return carry

            lax.fori_loop(0, outv.shape[0] // 16, emit, 0)
            emit_out(cb).start()

        return carry

    lax.fori_loop(0, blocks + 8, body, 0)

    def drain(j, carry):
        copy_c(j).wait_send()
        copy_t(j).wait_send()
        copy_ay(j).wait_send()
        copy_ax(j).wait_send()
        copy_af(j).wait_send()
        for k in range(4):
            copy_ac(j, k).wait_send()
        return carry

    lax.fori_loop(0, blocks, drain, 0)
    for k in range(steps_b):
        theirs_b(k).wait_send()
    for k in range(half_blocks):
        emit_out(k).wait()

    @pl.when(xpos == 0)
    def _():
        send_o().wait_send()


def finish(place, first, second, hidden, wv_heads, w_out, blocks, tag):
    mk, lk, uk, ux = first
    m0, l0, m1, l1, uo, us = second
    rows, half, rank = uk.shape
    vdim = wv_heads.shape[2]
    depth = half * vdim
    batch, dmodel = hidden.shape
    width = dmodel // (blocks // 2)
    vmem = pl.BlockSpec(memory_space=pltpu.VMEM)
    any_spec = pl.BlockSpec(memory_space=pl.ANY)
    ring = 2
    rows_b = 8
    steps_b = 2 * rows // rows_b
    f32 = jnp.float32
    return pl.pallas_call(
        finish_kernel,
        in_specs=[pl.BlockSpec(memory_space=pltpu.SMEM)] + [vmem] * 6 + [any_spec] * 7,
        out_specs=any_spec,
        out_shape=jax.ShapeDtypeStruct((batch, dmodel), jnp.bfloat16),
        scratch_shapes=[
            pltpu.VMEM((ring, depth, width), jnp.bfloat16),
            pltpu.VMEM((blocks, rows, width), f32),
            *[pltpu.VMEM((blocks, rows // 2, width), f32)] * 2,
            pltpu.VMEM((blocks, rows // 4, width), f32),
            pltpu.VMEM((blocks // 2, batch, width), f32),
            pltpu.VMEM((batch, width), f32),
            pltpu.VMEM((rows, depth), f32),
            pltpu.VMEM((rows, depth), jnp.bfloat16),
            pltpu.VMEM((2 * rows, depth), f32),
            pltpu.VMEM((rows, half, rank), f32),
            pltpu.VMEM((rows + 1, half, rank), f32),
            pltpu.VMEM((steps_b, rows_b, half, rank), f32),
            pltpu.VMEM((steps_b, rows_b, half, rank), f32),
            pltpu.VMEM((2, rows, half // 2, rank + 128), f32),
            pltpu.VMEM((half, rank, vdim), jnp.bfloat16),
            pltpu.VMEM((half, LANES), f32),
            pltpu.VMEM((half, LANES), f32),
            pltpu.VMEM((batch, dmodel), jnp.bfloat16),
            pltpu.VMEM((batch, dmodel), jnp.bfloat16),
            pltpu.SemaphoreType.DMA((ring,)),
            pltpu.SemaphoreType.DMA((2, 1, 1)),
            *[pltpu.SemaphoreType.DMA((2, 1, blocks))] * 5,
            pltpu.SemaphoreType.DMA((2, 4, blocks)),
            pltpu.SemaphoreType.DMA((2,)),
            pltpu.SemaphoreType.DMA((steps_b,)),
            pltpu.SemaphoreType.DMA((2, 1, steps_b)),
            pltpu.SemaphoreType.DMA((2, 1, 2)),
            pltpu.SemaphoreType.DMA,
            pltpu.SemaphoreType.DMA,
            pltpu.SemaphoreType.DMA((blocks // 2,)),
        ],
        compiler_params=pltpu.CompilerParams(collective_id=tag, has_side_effects=True, vmem_limit_bytes=VMEM_BYTES),
        name='finish_%d' % tag,
    )(place, mk, lk, m0, l0, m1, l1, uk, ux, uo, us, wv_heads, hidden, w_out)


def pair_kernel(m0_ref, l0_ref, m1_ref, l1_ref, uo_hbm, us_hbm, wuv_hbm, keep_ref, send_ref, m_ref, l_ref, wvh_ref, got, own, mg, lg, wv, wv_wide, ml_sem, d_sem, o_sem, v_sem):
    blocks, rows = own.shape[0], own.shape[1]
    sp = lax.axis_index('sp')
    xpos = sp // 2
    sib = {'sp': sp + 1 - 2 * lax.rem(sp, 2)}
    mesh_id = pl.DeviceIdType.MESH

    def remote(src, dst, sems, j):
        return pltpu.make_async_remote_copy(src_ref=src, dst_ref=dst, send_sem=sems.at[0, j], recv_sem=sems.at[1, j], device_id=sib, device_id_type=mesh_id)

    def mine(j):
        return pltpu.make_async_copy(uo_hbm.at[pl.ds(j * rows, rows)], own.at[j], o_sem.at[j])

    def theirs(j):
        return remote(us_hbm.at[pl.ds(j * rows, rows)], got.at[j], d_sem, j)

    half = uo_hbm.shape[1]
    quad = half // 2
    core = lax.rem(sp, 2)
    get_wv = pltpu.make_async_copy(wuv_hbm.at[:, pl.ds(pl.multiple_of(core * half, half), half)], wv, v_sem)
    get_wv.start()
    barrier = pltpu.get_barrier_semaphore()
    pl.semaphore_signal(barrier, inc=1, device_id=sib, device_id_type=mesh_id)
    for j in range(blocks):
        mine(j).start()
    pl.semaphore_wait(barrier, 1)
    cm = remote(m1_ref, mg, ml_sem, 0)
    cl = remote(l1_ref, lg, ml_sem, 1)
    cm.start()
    cl.start()
    for j in range(blocks):
        theirs(j).start()
    get_wv.wait()
    for p in range(2):
        wv_wide[...] = wv[:, p * quad:(p + 1) * quad, :].astype(jnp.float32)
        for h in range(quad):
            wvh_ref[p * quad + h] = wv_wide[:, h, :].astype(jnp.bfloat16)
    cm.wait()
    cl.wait()
    m0, m1 = m0_ref[...], mg[...]
    m = jnp.maximum(m0, m1)
    a0 = jnp.exp(m0 - m)
    a1 = jnp.exp(m1 - m)
    m_ref[...] = m
    l = l0_ref[...] * a0 + lg[...] * a1
    l_ref[...] = l
    send_ref[blocks * rows // 2] = jnp.concatenate([m, l, m, l], axis=1)
    lanes = lax.broadcasted_iota(jnp.int32, (1, 128), 1)

    def merge_block(j, out_ref, first):
        mine(j).wait()
        theirs(j).wait_recv()
        for r in range(rows):
            hit = lanes == j * rows + r
            c0 = jnp.sum(jnp.where(hit, a0, 0.0), axis=1, keepdims=True)
            c1 = jnp.sum(jnp.where(hit, a1, 0.0), axis=1, keepdims=True)
            out_ref[first + r] = own[j, r] * c0 + got[j, r] * c1

    side = blocks // 2

    def body(j, carry):
        merge_block((1 - xpos) * side + j, send_ref, j * rows)
        merge_block(xpos * side + j, keep_ref, j * rows)
        return carry

    lax.fori_loop(0, side, body, 0)

    def drain(j, carry):
        theirs(j).wait_send()
        return carry

    lax.fori_loop(0, blocks, drain, 0)


def pair_merge(mo, lo, ms, ls, uo, us, w_uv, tag):
    count, half, rank = uo.shape
    vdim = w_uv.shape[2]
    rows = 8
    blocks = count // rows
    vmem = pl.BlockSpec(memory_space=pltpu.VMEM)
    any_spec = pl.BlockSpec(memory_space=pl.ANY)
    return pl.pallas_call(
        pair_kernel,
        in_specs=[vmem, vmem, vmem, vmem, any_spec, any_spec, any_spec],
        out_specs=[vmem, vmem, vmem, vmem, vmem],
        out_shape=[
            jax.ShapeDtypeStruct((count // 2, half, rank), jnp.float32),
            jax.ShapeDtypeStruct((count // 2 + 1, half, rank), jnp.float32),
            jax.ShapeDtypeStruct((half, LANES), jnp.float32),
            jax.ShapeDtypeStruct((half, LANES), jnp.float32),
            jax.ShapeDtypeStruct((half, rank, vdim), jnp.bfloat16),
        ],
        scratch_shapes=[
            pltpu.VMEM((blocks, rows, half, rank), jnp.float32),
            pltpu.VMEM((blocks, rows, half, rank), jnp.float32),
            pltpu.VMEM((half, LANES), jnp.float32),
            pltpu.VMEM((half, LANES), jnp.float32),
            pltpu.VMEM((rank, half, vdim), jnp.bfloat16),
            pltpu.VMEM((rank, half // 2, vdim), jnp.float32),
            pltpu.SemaphoreType.DMA((2, 2)),
            pltpu.SemaphoreType.DMA((2, blocks)),
            pltpu.SemaphoreType.DMA((blocks,)),
            pltpu.SemaphoreType.DMA,
        ],
        compiler_params=pltpu.CompilerParams(collective_id=tag, has_side_effects=True, vmem_limit_bytes=VMEM_BYTES - 4 * VMEM_STEP),
        name='pair_merge_%d' % tag,
    )(mo, lo, ms, ls, uo, us, w_uv)


def merge_tiles(m0, l0, u0, m1, l1, u1):
    m = jnp.maximum(m0, m1)
    a0 = jnp.exp(m0 - m)
    a1 = jnp.exp(m1 - m)
    count = u0.shape[0]
    return m, l0 * a0 + l1 * a1, u0 * a0[:, :count].T[:, :, None] + u1 * a1[:, :count].T[:, :, None]


def solution(mesh):
    row_spec = P('dp', None)
    cache_spec = P('dp', 'sp', None)
    head_spec = P(None, 'tp', None)
    in_specs = (row_spec, cache_spec, cache_spec, P('dp'), P(), P(), P(), P(), head_spec, head_spec, head_spec, P('tp', None))
    out_specs = (row_spec, cache_spec, cache_spec)
    sibling = [(0, 1), (1, 0), (2, 3), (3, 2)]
    across = [(0, 2), (2, 0), (1, 3), (3, 1)]

    def local_step(hidden, lat_cache, rope_cache, positions, w_dq, gain_q, w_dkv, gain_kv, w_uq, w_uk, w_uv, w_out):
        rows = hidden.shape[0]
        slots = lat_cache.shape[1]
        heads = w_uq.shape[1]
        half = heads // 2
        scale = YARN_MSCALE ** 2 / math.sqrt(w_uq.shape[2])
        sp = lax.axis_index('sp')
        core = sp % 2
        xpos = sp // 2
        ids = jnp.arange(rows, dtype=jnp.int32)
        ahead = (positions[None, :] > positions[:, None]) | ((positions[None, :] == positions[:, None]) & (ids[None, :] < ids[:, None]))
        rank_of = jnp.sum(ahead.astype(jnp.int32), axis=1)
        pick = rank_of[None, :] == ids[:, None]
        order = jnp.sum(jnp.where(pick, ids[None, :], 0), axis=1)
        pos = jnp.sum(jnp.where(pick, positions[None, :], 0), axis=1)
        cos_t, sin_t = rope_tables(pos, rope_cache.shape[2])
        cos2 = jnp.concatenate([cos_t, cos_t], axis=1)
        sin2 = jnp.concatenate([sin_t, sin_t], axis=1)
        cq, latn, ropen = down_project(order, hidden, w_dq, jnp.transpose(w_dkv), gain_q, gain_kv, cos2, sin2)
        rope_t = jnp.swapaxes(rope_cache, 1, 2)
        where = jnp.stack([sp * slots, core]).astype(jnp.int32)
        q_abs, q_rope = head_queries(cq, cos2, sin2, jnp.transpose(w_uq, (1, 2, 0)), w_uk)

        half_rows = rows // 2
        own_rows = rows // 4
        args = (scale, order, pos)
        uo, us, mo, lo, ms, ls, *held = attend_chunk(0, half_rows, *args, where, q_abs, q_rope, latn, ropen, lat_cache, rope_t, [])
        keep, send, mk, lk, wv_heads = pair_merge(mo, lo, ms, ls, uo, us, w_uv, 2)
        where, send = lax.optimization_barrier((where, send))
        ux = lax.ppermute(send, 'sp', across)
        uo, us, mo, lo, ms, ls, lat_out, rope_n = attend_chunk(half_rows, half_rows, *args, where, q_abs, q_rope, latn, ropen, lat_cache, rope_t, held)
        rope_out = jnp.swapaxes(rope_n, 1, 2)
        r = rank_of % half_rows
        x, k = r // own_rows, r % own_rows
        quarter = own_rows // 4
        c, t = k // (2 * quarter), (k // quarter) % 2
        place = (rank_of // half_rows) * half_rows + ((x * 2 + c) * 2 + t) * quarter + k % quarter
        place = place.astype(jnp.int32)

        def far(_, second):
            m0, l0, m1, l1, u0, u1 = second
            gm0, gl0, gm1, gl1, gu0, gu1 = lax.ppermute(second, 'sp', across)
            m0, l0, u0 = merge_tiles(m0, l0, u0, gm0, gl0, gu0)
            m1, l1, u1 = merge_tiles(m1, l1, u1, gm1, gl1, gu1)
            return m0, l0, m1, l1, u0, u1

        trips = (pos[half_rows] >= 2 * slots).astype(jnp.int32)
        ux, uo = lax.optimization_barrier((ux, uo))
        second = lax.fori_loop(0, trips, far, (mo, lo, ms, ls, uo, us))
        out = finish(place, (mk, lk, keep, ux), second, hidden, wv_heads, w_out, 12, 3)
        return out, lat_out, rope_out

    return jax.shard_map(local_step, mesh=mesh, in_specs=in_specs, out_specs=out_specs, check_vma=False)
```

```python
import functools
import math
import jax
import jax.numpy as jnp
from jax import lax
from jax.experimental import pallas as pl
from jax.experimental.pallas import tpu as pltpu
from jax.sharding import PartitionSpec as P

EPSILON = 1e-6
ROPE_BASE = 50000.0
YARN_MSCALE = 1.0 + 0.1 * math.log(32.0)
MASK_VALUE = -1e30
GROUP = 8
RING = 4
AHEAD = 2
VIA_Y = 0
SHIP = 2
LANES = 128
PACK = 16
VMEM_BYTES = 67043328
VMEM_STEP = 1048576


def rope_tables(positions, rope_dim):
    half_dim = rope_dim // 2
    inv_freq = ROPE_BASE ** (-jnp.arange(half_dim).astype(jnp.float32) / half_dim)
    angles = positions.astype(jnp.float32)[:, None] * inv_freq[None, :]
    return jnp.cos(angles), jnp.sin(angles)


def insert_slot(i, start, pos_ref, latn_ref, ropen_ref, lat, rope):
    slots = lat.shape[0]
    rdim = rope.shape[0]
    s = pos_ref[i] - start
    inside = jnp.logical_and(s >= 0, s < slots)
    sc = jnp.where(inside, s, 0)
    r0 = pl.multiple_of((sc // PACK) * PACK, PACK)
    hit = lax.broadcasted_iota(jnp.int32, (PACK, 1), 0) == jnp.where(inside, sc - r0, -1)
    blk = lat[pl.ds(r0, PACK), :]
    lat[pl.ds(r0, PACK), :] = jnp.where(hit, latn_ref[pl.ds(i, 1), :], blk.astype(jnp.float32)).astype(jnp.bfloat16)
    c0 = pl.multiple_of((sc // LANES) * LANES, LANES)
    hit = lax.broadcasted_iota(jnp.int32, (1, LANES), 1) == jnp.where(inside, sc - c0, -1)
    eye = lax.broadcasted_iota(jnp.int32, (rdim, rdim), 0) == lax.broadcasted_iota(jnp.int32, (rdim, rdim), 1)
    col = jnp.sum(jnp.where(eye, ropen_ref[pl.ds(i, 1), :], 0.0), axis=1, keepdims=True)
    blk = rope[:, pl.ds(c0, LANES)]
    rope[:, pl.ds(c0, LANES)] = jnp.where(hit, col, blk.astype(jnp.float32)).astype(jnp.bfloat16)


def heads_kernel(cq_ref, cos_ref, sin_ref, wuq_ref, wuk_ref, qa_ref, qr_ref, wide, lines, rlines):
    block = wuq_ref.shape[0]
    nope = wuk_ref.shape[2]
    rank = wuk_ref.shape[0]
    rdim = wuq_ref.shape[1] - nope
    hdim = rdim // 2
    wide[...] = wuk_ref[...].astype(jnp.float32)
    cq = cq_ref[...]
    depth = cq.shape[1]
    dims = (((1,), (1,)), ((), ()))
    w_rope = wuq_ref[:, nope:, :].reshape(block * rdim, depth)
    r = lax.dot_general(cq, w_rope, dims, preferred_element_type=jnp.float32).astype(jnp.bfloat16).astype(jnp.float32)
    lane = lax.broadcasted_iota(jnp.int32, (1, block * rdim), 1)
    width = block * rdim
    turned = jnp.where(lane % rdim < hdim, -pltpu.roll(r, width - hdim, 1), pltpu.roll(r, hdim, 1))
    r = r * jnp.concatenate([cos_ref[...]] * block, axis=1) + turned * jnp.concatenate([sin_ref[...]] * block, axis=1)
    w_nope = wuq_ref[:, :nope, :].reshape(block * nope, depth)
    q = lax.dot_general(cq, w_nope, dims, preferred_element_type=jnp.float32).astype(jnp.bfloat16)
    for h in range(block):
        rlines[:, h, :rdim] = r[:, h * rdim:(h + 1) * rdim]
        wk = wide[:, h, :].astype(jnp.bfloat16)
        lines[:, h, :rank] = lax.dot_general(q[:, h * nope:(h + 1) * nope], wk, dims, preferred_element_type=jnp.float32)
    qa_ref[...] = lines[:, :, :rank].astype(jnp.bfloat16)
    qr_ref[...] = rlines[:, :, :rdim].astype(jnp.bfloat16)


def head_queries(cq, cos2, sin2, w_uq_t, w_uk):
    rows, qrank = cq.shape
    heads, qdim, _ = w_uq_t.shape
    rank, _, nope = w_uk.shape
    rdim = qdim - nope
    block = GROUP
    f32 = jnp.float32
    whole = lambda v: pl.BlockSpec(v.shape, lambda i: (0, 0))
    return pl.pallas_call(
        heads_kernel,
        grid=(heads // block,),
        in_specs=[
            whole(cq), whole(cos2), whole(sin2),
            pl.BlockSpec((block, qdim, qrank), lambda i: (i, 0, 0)),
            pl.BlockSpec((rank, block, nope), lambda i: (0, i, 0)),
        ],
        out_specs=[pl.BlockSpec((rows, block, d), lambda i: (0, i, 0)) for d in (rank, rdim)],
        out_shape=[jax.ShapeDtypeStruct((rows, heads, d), jnp.bfloat16) for d in (rank, rdim)],
        scratch_shapes=[
            pltpu.VMEM((rank, block, nope), f32),
            pltpu.VMEM((rows, block, rank + LANES), f32),
            pltpu.VMEM((rows, block, LANES), f32),
        ],
        compiler_params=pltpu.CompilerParams(dimension_semantics=('arbitrary',), vmem_limit_bytes=VMEM_BYTES - 8 * VMEM_STEP),
        cost_estimate=pl.CostEstimate(flops=2 * rows * heads * (qdim * qrank + nope * rank), bytes_accessed=2 * heads * (qdim * qrank + nope * rank), transcendentals=0),
        name='head_queries',
    )(cq, cos2, sin2, w_uq_t, w_uk)


def down_kernel(rank_ref, hid_ref, wdq_ref, wkv_ref, gq_ref, gkv_ref, cos_ref, sin_ref, cq_ref, latn_ref, ropen_ref, pick, acc_q, acc_kv):
    i = pl.program_id(0)
    rows = hid_ref.shape[0]
    rank = gkv_ref.shape[0]
    hdim = cos_ref.shape[1] // 2

    @pl.when(i == 0)
    def _():
        pick[...] = (rank_ref[...][None, :] == lax.broadcasted_iota(jnp.int32, (rows, rows), 0)).astype(jnp.bfloat16)
        acc_q[...] = jnp.zeros_like(acc_q)
        acc_kv[...] = jnp.zeros_like(acc_kv)

    x = jnp.dot(pick[...], hid_ref[...], preferred_element_type=jnp.float32).astype(jnp.bfloat16)
    acc_q[...] += jnp.dot(x, wdq_ref[...], preferred_element_type=jnp.float32)
    acc_kv[...] += lax.dot_general(x, wkv_ref[...], (((1,), (1,)), ((), ())), preferred_element_type=jnp.float32)

    @pl.when(i == pl.num_programs(0) - 1)
    def _():
        def normed(v, gain):
            v = v.astype(jnp.bfloat16).astype(jnp.float32)
            inv = lax.rsqrt(jnp.mean(v * v, axis=-1, keepdims=True) + EPSILON)
            return (v * inv * gain.astype(jnp.float32)[None, :]).astype(jnp.bfloat16)

        cq_ref[...] = normed(acc_q[...], gq_ref[...])
        latn_ref[...] = normed(acc_kv[:, :rank], gkv_ref[...]).astype(jnp.float32)
        r = acc_kv[:, rank:].astype(jnp.bfloat16).astype(jnp.float32)
        turned = jnp.concatenate([-r[:, hdim:], r[:, :hdim]], axis=1)
        ropen_ref[...] = (r * cos_ref[...] + turned * sin_ref[...]).astype(jnp.bfloat16).astype(jnp.float32)


def down_project(rank_of, hidden, w_dq, w_dkv_t, gain_q, gain_kv, cos2, sin2):
    rows, dmodel = hidden.shape
    qrank = w_dq.shape[1]
    width = w_dkv_t.shape[0]
    rank = gain_kv.shape[0]
    block = 1024
    fixed = lambda i: (0, 0)
    return pl.pallas_call(
        down_kernel,
        grid=(dmodel // block,),
        in_specs=[
            pl.BlockSpec((rows,), lambda i: (0,)),
            pl.BlockSpec((rows, block), lambda i: (0, i)),
            pl.BlockSpec((block, qrank), lambda i: (i, 0)),
            pl.BlockSpec((width, block), lambda i: (0, i)),
            pl.BlockSpec((qrank,), lambda i: (0,)),
            pl.BlockSpec((rank,), lambda i: (0,)),
            pl.BlockSpec(cos2.shape, fixed),
            pl.BlockSpec(sin2.shape, fixed),
        ],
        out_specs=[pl.BlockSpec((rows, qrank), fixed), pl.BlockSpec((rows, rank), fixed), pl.BlockSpec((rows, width - rank), fixed)],
        out_shape=[
            jax.ShapeDtypeStruct((rows, qrank), jnp.bfloat16),
            jax.ShapeDtypeStruct((rows, rank), jnp.float32),
            jax.ShapeDtypeStruct((rows, width - rank), jnp.float32),
        ],
        scratch_shapes=[
            pltpu.VMEM((rows, rows), jnp.bfloat16),
            pltpu.VMEM((rows, qrank), jnp.float32),
            pltpu.VMEM((rows, width), jnp.float32),
        ],
        compiler_params=pltpu.CompilerParams(dimension_semantics=('arbitrary',), vmem_limit_bytes=VMEM_BYTES - 8 * VMEM_STEP),
        cost_estimate=pl.CostEstimate(flops=2 * rows * dmodel * (qrank + width + rows), bytes_accessed=2 * dmodel * (qrank + width), transcendentals=0),
        name='down_project',
    )(rank_of, hidden, w_dq, w_dkv_t, gain_q, gain_kv, cos2, sin2)


def attend_kernel(first, steps, scale, order_ref, pos_ref, where_ref, qa_ref, qr_ref, latn_ref, ropen_ref, lat_hbm, rope_hbm, *rest):
    uo_ref, us_ref, mo_ref, lo_ref, ms_ref, ls_ref, lat_out, rope_out, lat_buf, rope_buf, in_sem, out_sem = rest[-12:]
    t = pl.program_id(0)
    slots = lat_buf.shape[2]
    heads = qa_ref.shape[1]
    half = heads // 2
    start = where_ref[0]
    own = where_ref[1]

    def reads(step):
        ring = lax.rem(step, RING)
        out = []
        for g in range(GROUP):
            b = order_ref[first + step * GROUP + g]
            out.append(pltpu.make_async_copy(lat_hbm.at[b], lat_buf.at[ring, g], in_sem.at[ring, g, 0]))
            out.append(pltpu.make_async_copy(rope_hbm.at[b], rope_buf.at[ring, g], in_sem.at[ring, g, 1]))
        return out

    def writes(step):
        ring = lax.rem(step, RING)
        out = []
        for g in range(GROUP):
            b = order_ref[first + step * GROUP + g]
            out.append(pltpu.make_async_copy(lat_buf.at[ring, g], lat_out.at[b], out_sem.at[ring, g, 0]))
            out.append(pltpu.make_async_copy(rope_buf.at[ring, g], rope_out.at[b], out_sem.at[ring, g, 1]))
        return out

    @pl.when(t == 0)
    def _():
        for s in range(min(AHEAD, steps)):
            for c in reads(s):
                c.start()

    lag = RING - AHEAD

    @pl.when(t >= lag)
    def _():
        for c in writes(t - lag):
            c.wait()

    @pl.when(t + AHEAD < steps)
    def _():
        for c in reads(t + AHEAD):
            c.start()

    for c in reads(t):
        c.wait()

    ring = lax.rem(t, RING)
    lanes = lax.broadcasted_iota(jnp.int32, (1, LANES), 1)
    for g in range(GROUP):
        insert_slot(first + t * GROUP + g, start, pos_ref, latn_ref, ropen_ref, lat_buf.at[ring, g], rope_buf.at[ring, g])

    slot_ids = lax.broadcasted_iota(jnp.int32, (1, slots), 1) + start
    o0 = pl.multiple_of(own * half, half)
    o1 = pl.multiple_of((1 - own) * half, half)
    scores = []
    for g in range(GROUP):
        i = first + t * GROUP + g
        qa = jnp.concatenate([qa_ref[g, pl.ds(o0, half), :], qa_ref[g, pl.ds(o1, half), :]], axis=0)
        qr = jnp.concatenate([qr_ref[g, pl.ds(o0, half), :], qr_ref[g, pl.ds(o1, half), :]], axis=0)
        s = lax.dot_general(qa, lat_buf[ring, g], (((1,), (1,)), ((), ())), preferred_element_type=jnp.float32)
        s = (s + jnp.dot(qr, rope_buf[ring, g], preferred_element_type=jnp.float32)) * scale
        scores.append(jnp.where(slot_ids <= pos_ref[i], s, MASK_VALUE))
    ms = jnp.concatenate([mo_ref[...], ms_ref[...]], axis=0)
    ls = jnp.concatenate([lo_ref[...], ls_ref[...]], axis=0)
    for g in range(GROUP):
        i = first + t * GROUP + g
        m = jnp.max(scores[g], axis=1, keepdims=True)
        p = jnp.where(slot_ids <= pos_ref[i], jnp.exp(scores[g] - m), 0.0)
        l = jnp.sum(p, axis=1, keepdims=True)
        u = jnp.dot(p.astype(jnp.bfloat16), lat_buf[ring, g], preferred_element_type=jnp.float32)
        uo_ref[g] = u[:half]
        us_ref[g] = u[half:]
        j = t * GROUP + g
        ms = jnp.where(lanes == j, m, ms)
        ls = jnp.where(lanes == j, l, ls)
    mo_ref[...] = ms[:half]
    lo_ref[...] = ls[:half]
    ms_ref[...] = ms[half:]
    ls_ref[...] = ls[half:]

    for c in writes(t):
        c.start()

    @pl.when(t == steps - 1)
    def _():
        for s in range(max(0, steps - lag), steps):
            for c in writes(s):
                c.wait()


def attend_chunk(first, count, scale, order, pos, where, qa, qr, latn, ropen, lat, rope, prev):
    steps = count // GROUP
    heads, rank = qa.shape[1:]
    rdim = qr.shape[2]
    slots = lat.shape[1]
    half = heads // 2
    base = first // GROUP
    any_spec = pl.BlockSpec(memory_space=pl.ANY)
    fixed = lambda t, *_: (0, 0)
    bf16, f32 = jnp.bfloat16, jnp.float32
    dma = pltpu.SemaphoreType.DMA((RING, GROUP, 2))
    part = jax.ShapeDtypeStruct((count, half, rank), f32)
    tile = jax.ShapeDtypeStruct((half, LANES), f32)
    return pl.pallas_call(
        functools.partial(attend_kernel, first, steps, scale),
        grid_spec=pltpu.PrefetchScalarGridSpec(
            num_scalar_prefetch=3,
            grid=(steps,),
            in_specs=[pl.BlockSpec((GROUP, heads, d), lambda t, *_: (base + t, 0, 0)) for d in (rank, rdim)]
            + [pl.BlockSpec(v.shape, fixed) for v in (latn, ropen)] + [any_spec] * (2 + len(prev)),
            out_specs=[pl.BlockSpec((GROUP, half, rank), lambda t, *_: (t, 0, 0))] * 2 + [pl.BlockSpec(tile.shape, fixed)] * 4 + [any_spec] * 2,
            scratch_shapes=[
                pltpu.VMEM((RING, GROUP, slots, rank), bf16),
                pltpu.VMEM((RING, GROUP, rdim, slots), bf16),
                dma, dma,
            ],
        ),
        out_shape=[part] * 2 + [tile] * 4 + [jax.ShapeDtypeStruct(v.shape, bf16) for v in (lat, rope)],
        input_output_aliases={9: 6, 10: 7} if prev else {},
        compiler_params=pltpu.CompilerParams(dimension_semantics=('arbitrary',), vmem_limit_bytes=VMEM_BYTES - 8 * VMEM_STEP),
        cost_estimate=pl.CostEstimate(
            flops=64 * count * heads * slots * rank, bytes_accessed=count * slots * (rank + rdim) * 4, transcendentals=0),
        name='attend_chunk_%d' % first,
    )(order, pos, where, qa, qr, latn, ropen, lat, rope, *prev)


def finish_kernel(place_ref, mk_ref, lk_ref, m0_ref, l0_ref, m1_ref, l1_ref, uk_hbm, ux_hbm, uo_hbm, us_hbm, wvh_hbm, hid_hbm, w_hbm, out_hbm, wbuf, part, got_c, sum_c, got_t, full, staged, o_got, o1, o2, ua, ux, ub, ud, un, wv_heads, mg, lg, hid, outv, w_sem, o_sem, c_sem, t_sem, ay_sem, ax_sem, af_sem, ac_sem, a_sem, b_sem, d_sem, ml_sem, v_sem, h_sem, r_sem):
    blocks, rows, width = part.shape
    half_blocks = blocks // 2
    r2, r4 = rows // 2, rows // 4
    depth = wbuf.shape[1]
    sp = lax.axis_index('sp')
    tp = lax.axis_index('tp')
    core = lax.rem(sp, 2)
    xpos = sp // 2
    sib = {'sp': sp + 1 - 2 * core}
    nbx = {'sp': lax.rem(sp + 2, 4)}
    nby = {'tp': 1 - tp}
    mesh_id = pl.DeviceIdType.MESH

    def remote(src, dst, sems, j, to, k=0):
        return pltpu.make_async_remote_copy(src_ref=src, dst_ref=dst, send_sem=sems.at[0, k, j], recv_sem=sems.at[1, k, j], device_id=to, device_id_type=mesh_id)

    def wcopy(j):
        col = lax.rem(j, half_blocks)
        return pltpu.make_async_copy(
            w_hbm.at[pl.ds(pl.multiple_of(core * depth, depth), depth), pl.ds(pl.multiple_of(col * width, width), width)],
            wbuf.at[lax.rem(j, wbuf.shape[0])], w_sem.at[lax.rem(j, wbuf.shape[0])])

    def spot(j, x, c, t):
        first = pl.multiple_of((j // half_blocks) * 4 * rows // 2 + ((x * 2 + c) * 2 + t) * r4, r4)
        return full.at[lax.rem(j, half_blocks), pl.ds(first, r4)]

    pieces = o_sem.shape[-1]
    share = rows // pieces

    def send_o(k):
        first = pl.multiple_of(k * share, share)
        return remote(o2.at[pl.ds(rows + first, share)], o_got.at[pl.ds(first, share)], o_sem, k, nbx)

    def copy_c(j):
        return remote(part.at[j, pl.ds(pl.multiple_of((1 - core) * r2, r2), r2)], got_c.at[j], c_sem, j, sib)

    def copy_t(j):
        return remote(sum_c.at[j, pl.ds(pl.multiple_of((1 - tp) * r4, r4), r4)], got_t.at[j], t_sem, j, nby)

    def copy_ay(j):
        return remote(spot(j, xpos, core, tp), spot(j, xpos, core, tp), ay_sem, j, nby)

    def copy_ax(j):
        return remote(spot(j, xpos, core, tp), spot(j, xpos, core, tp), ax_sem, j, nbx)

    def copy_af(j):
        return remote(spot(j, xpos, core, 1 - tp), spot(j, xpos, core, 1 - tp), af_sem, j, nbx)

    def copy_ag(j):
        return remote(spot(j, 1 - xpos, core, tp), spot(j, 1 - xpos, core, tp), af_sem, j, nby)

    via_y = VIA_Y

    def emit_out(cb):
        cols = pl.ds(pl.multiple_of(cb * width, width), width)
        return pltpu.make_async_copy(outv.at[:, cols], out_hbm.at[:, cols], r_sem.at[cb])

    def copy_ac(j, k):
        x = xpos if k < 2 else 1 - xpos
        t = tp if k % 2 == 0 else 1 - tp
        return remote(spot(j, x, core, t), spot(j, x, core, t), ac_sem, j, sib, k)

    half = uk_hbm.shape[1]
    vdim = wvh_hbm.shape[2]
    quad = half // 2
    steps_b = ud.shape[0]
    rows_b = ud.shape[1]
    side_b = steps_b // 2

    def mine_a(k):
        if k == 0:
            return pltpu.make_async_copy(uk_hbm, ua, a_sem.at[0])
        return pltpu.make_async_copy(ux_hbm, ux, a_sem.at[1])

    def mine_b(k):
        return pltpu.make_async_copy(uo_hbm.at[pl.ds(k * rows_b, rows_b)], ub.at[k], b_sem.at[k])

    def theirs_b(k):
        return remote(us_hbm.at[pl.ds(k * rows_b, rows_b)], ud.at[k], d_sem, k, sib)

    get_wv = pltpu.make_async_copy(wvh_hbm, wv_heads, v_sem)
    get_hid = pltpu.make_async_copy(hid_hbm, hid, h_sem)
    order_b = list(range(side_b, steps_b)) + list(range(side_b))
    for k in range(2):
        mine_a(k).start()
    get_wv.start()
    for j in range(wbuf.shape[0] - 1):
        wcopy(j).start()
    for k in order_b:
        mine_b(k).start()
    get_hid.start()
    barrier = pltpu.get_barrier_semaphore()
    for to in (sib, nbx, nby):
        pl.semaphore_signal(barrier, inc=1, device_id=to, device_id_type=mesh_id)
    pl.semaphore_wait(barrier, 3)
    tiles = [remote(src, dst, ml_sem, k, sib) for k, (src, dst) in enumerate(((m1_ref, mg), (l1_ref, lg)))]
    for c in tiles:
        c.start()
    for k in order_b:
        theirs_b(k).start()

    lanes = lax.broadcasted_iota(jnp.int32, (1, 128), 1)

    def weights(m0, l0, m1, l1):
        m = jnp.maximum(m0, m1)
        a0 = jnp.exp(m0 - m)
        a1 = jnp.exp(m1 - m)
        l = l0 * a0 + l1 * a1
        inv = 1.0 / jnp.where(l > 0, l, 1.0)
        return a0 * inv, a1 * inv

    def merge_row(w, lane, first, second, to):
        hit = lanes == lane
        c0 = jnp.sum(jnp.where(hit, w[0], 0.0), axis=1, keepdims=True)
        c1 = jnp.sum(jnp.where(hit, w[1], 0.0), axis=1, keepdims=True)
        u = first * c0 + second * c1
        un[0, to, :, :u.shape[1]] = u[:quad]
        un[1, to, :, :u.shape[1]] = u[quad:]

    rank = uk_hbm.shape[2]

    def heads_out(to, first):
        def one(h, carry):
            for p in range(2):
                u = un[p, :, h, :rank].astype(jnp.bfloat16)
                o = jnp.dot(u, wv_heads[p * quad + h], preferred_element_type=jnp.float32)
                to[pl.ds(first, rows), pl.ds(pl.multiple_of((p * quad + h) * vdim, vdim), vdim)] = o.astype(to.dtype)
            return carry
        for h in range(quad):
            one(h, 0)

    def rows_of(k, q):
        mine_b(k).wait()
        theirs_b(k).wait_recv()
        w = weights(m0_ref[...], l0_ref[...], mg[...], lg[...])
        for e in range(rows_b):
            merge_row(w, k * rows_b + e, ub[k, e], ud[k, e], pl.multiple_of(q * rows_b, rows_b) + e)

    def first_side(q, carry):
        rows_of(side_b + q, q)
        return carry

    for k in range(2):
        mine_a(k).wait()
    wa = weights(mk_ref[...], lk_ref[...], ux[rows, :, :128], ux[rows, :, 128:256])

    def rows_a(q, carry):
        for e in range(8):
            r = q * 8 + e
            merge_row(wa, xpos * rows + r, ua[r], ux[r], r)
        return carry

    lax.fori_loop(0, rows // 8, rows_a, 0)
    get_wv.wait()
    heads_out(o1, 0)
    for c in tiles:
        c.wait()

    def second_group(i):
        per = side_b // 2

        @pl.when(i == 1)
        def _():
            lax.fori_loop(0, side_b, first_side, 0)
            heads_out(o2, rows)

        @pl.when(jnp.logical_and(xpos == 0, jnp.logical_and(i >= 1, i <= pieces // SHIP)))
        def _():
            for e in range(SHIP):
                send_o((i - 1) * SHIP + e).start()

        @pl.when(jnp.logical_and(i >= 3, i < 5))
        def _():
            def one(e, carry):
                q = (i - 3) * per + e
                rows_of(q, q)
                return carry

            lax.fori_loop(0, per, one, 0)

        @pl.when(i == 4)
        def _():
            heads_out(o2, 0)

    def body(i, carry):
        j = i

        @pl.when(j < blocks)
        def _():
            @pl.when(jnp.logical_and(j == half_blocks, xpos == 1))
            def _():
                for k in range(pieces):
                    send_o(k).wait_recv()

            wcopy(j).wait()
            w = wbuf.at[lax.rem(j, wbuf.shape[0])]

            @pl.when(j < half_blocks)
            def _():
                part[j] = jnp.dot(o1[...], w[...], preferred_element_type=jnp.float32)

            @pl.when(j >= half_blocks)
            def _():
                o = jnp.where(xpos == 0, o2[pl.ds(0, rows)], o_got[...])
                part[j] = jnp.dot(o.astype(jnp.bfloat16), w[...], preferred_element_type=jnp.float32)

            @pl.when(j + wbuf.shape[0] - 1 < blocks)
            def _():
                wcopy(j + wbuf.shape[0] - 1).start()

            copy_c(j).start()

        j1 = i - 1

        @pl.when(jnp.logical_and(j1 >= 0, j1 < blocks))
        def _():
            copy_c(j1).wait_recv()
            sum_c[j1] = part[j1, pl.ds(pl.multiple_of(core * r2, r2), r2)] + got_c[j1]
            copy_t(j1).start()

        second_group(i)

        j2 = i - 3

        @pl.when(jnp.logical_and(j2 >= 0, j2 < blocks))
        def _():
            copy_t(j2).wait_recv()
            first = pl.multiple_of((j2 // half_blocks) * 2 * rows + ((xpos * 2 + core) * 2 + tp) * r4, r4)
            full[lax.rem(j2, half_blocks), pl.ds(first, r4)] = sum_c[j2, pl.ds(pl.multiple_of(tp * r4, r4), r4)] + got_t[j2]
            copy_ay(j2).start()
            copy_ax(j2).start()
            copy_ac(j2, 0).start()

        j3 = i - 5

        @pl.when(jnp.logical_and(j3 >= 0, j3 < blocks))
        def _():
            copy_ay(j3).wait_recv()

            @pl.when(j3 >= via_y)
            def _():
                copy_af(j3).start()

            copy_ac(j3, 1).start()
            copy_ax(j3).wait_recv()

            @pl.when(j3 < via_y)
            def _():
                copy_ag(j3).start()

            copy_ac(j3, 2).start()

        j4 = i - 7

        @pl.when(jnp.logical_and(j4 >= 0, j4 < blocks))
        def _():
            copy_af(j4).wait_recv()
            copy_ac(j4, 3).start()

        j5 = i - 8

        @pl.when(jnp.logical_and(j5 >= 0, j5 < blocks))
        def _():
            for k in range(4):
                copy_ac(j5, k).wait_recv()

        @pl.when(jnp.logical_and(j5 >= half_blocks, j5 < blocks))
        def _():
            cb = j5 - half_blocks
            cols = pl.ds(pl.multiple_of(cb * width, width), width)
            staged[...] = full[cb]

            @pl.when(cb == 0)
            def _():
                get_hid.wait()


            def emit(q, carry):
                b = pl.multiple_of(q * 16, 16)
                lines = [staged[pl.ds(place_ref[b + r], 1), :] for r in range(16)]
                y = jnp.concatenate(lines, axis=0)
                outv[pl.ds(b, 16), cols] = (hid[pl.ds(b, 16), cols].astype(jnp.float32) + y).astype(jnp.bfloat16)
                return carry

            lax.fori_loop(0, outv.shape[0] // 16, emit, 0)
            emit_out(cb).start()

        return carry

    lax.fori_loop(0, blocks + 8, body, 0)

    def drain(j, carry):
        copy_c(j).wait_send()
        copy_t(j).wait_send()
        copy_ay(j).wait_send()
        copy_ax(j).wait_send()
        copy_af(j).wait_send()
        for k in range(4):
            copy_ac(j, k).wait_send()
        return carry

    lax.fori_loop(0, blocks, drain, 0)
    for k in range(steps_b):
        theirs_b(k).wait_send()
    for k in range(half_blocks):
        emit_out(k).wait()

    @pl.when(xpos == 0)
    def _():
        for k in range(pieces):
            send_o(k).wait_send()


def finish(place, first, second, hidden, wv_heads, w_out, blocks, tag):
    mk, lk, uk, ux = first
    m0, l0, m1, l1, uo, us = second
    rows, half, rank = uk.shape
    vdim = wv_heads.shape[2]
    depth = half * vdim
    batch, dmodel = hidden.shape
    width = dmodel // (blocks // 2)
    vmem = pl.BlockSpec(memory_space=pltpu.VMEM)
    any_spec = pl.BlockSpec(memory_space=pl.ANY)
    ring = 2
    rows_b = 8
    steps_b = 2 * rows // rows_b
    f32 = jnp.float32
    return pl.pallas_call(
        finish_kernel,
        in_specs=[pl.BlockSpec(memory_space=pltpu.SMEM)] + [vmem] * 6 + [any_spec] * 7,
        out_specs=any_spec,
        out_shape=jax.ShapeDtypeStruct((batch, dmodel), jnp.bfloat16),
        scratch_shapes=[
            pltpu.VMEM((ring, depth, width), jnp.bfloat16),
            pltpu.VMEM((blocks, rows, width), f32),
            *[pltpu.VMEM((blocks, rows // 2, width), f32)] * 2,
            pltpu.VMEM((blocks, rows // 4, width), f32),
            pltpu.VMEM((blocks // 2, batch, width), f32),
            pltpu.VMEM((batch, width), f32),
            pltpu.VMEM((rows, depth), f32),
            pltpu.VMEM((rows, depth), jnp.bfloat16),
            pltpu.VMEM((2 * rows, depth), f32),
            pltpu.VMEM((rows, half, rank), f32),
            pltpu.VMEM((rows + 1, half, rank), f32),
            pltpu.VMEM((steps_b, rows_b, half, rank), f32),
            pltpu.VMEM((steps_b, rows_b, half, rank), f32),
            pltpu.VMEM((2, rows, half // 2, rank + 128), f32),
            pltpu.VMEM((half, rank, vdim), jnp.bfloat16),
            pltpu.VMEM((half, LANES), f32),
            pltpu.VMEM((half, LANES), f32),
            pltpu.VMEM((batch, dmodel), jnp.bfloat16),
            pltpu.VMEM((batch, dmodel), jnp.bfloat16),
            pltpu.SemaphoreType.DMA((ring,)),
            pltpu.SemaphoreType.DMA((2, 1, 8)),
            *[pltpu.SemaphoreType.DMA((2, 1, blocks))] * 5,
            pltpu.SemaphoreType.DMA((2, 4, blocks)),
            pltpu.SemaphoreType.DMA((2,)),
            pltpu.SemaphoreType.DMA((steps_b,)),
            pltpu.SemaphoreType.DMA((2, 1, steps_b)),
            pltpu.SemaphoreType.DMA((2, 1, 2)),
            pltpu.SemaphoreType.DMA,
            pltpu.SemaphoreType.DMA,
            pltpu.SemaphoreType.DMA((blocks // 2,)),
        ],
        compiler_params=pltpu.CompilerParams(collective_id=tag, has_side_effects=True, vmem_limit_bytes=VMEM_BYTES),
        name='finish_%d' % tag,
    )(place, mk, lk, m0, l0, m1, l1, uk, ux, uo, us, wv_heads, hidden, w_out)


def pair_kernel(m0_ref, l0_ref, m1_ref, l1_ref, uo_hbm, us_hbm, wuv_hbm, m_ref, l_ref, keep_hbm, send_hbm, wvh_hbm, got, own, mg, lg, wv, wv_wide, wvh, extra, ml_sem, d_sem, o_sem, v_sem, r_sem, e_sem):
    blocks, rows = own.shape[0], own.shape[1]
    sp = lax.axis_index('sp')
    xpos = sp // 2
    sib = {'sp': sp + 1 - 2 * lax.rem(sp, 2)}
    mesh_id = pl.DeviceIdType.MESH

    def remote(src, dst, sems, j):
        return pltpu.make_async_remote_copy(src_ref=src, dst_ref=dst, send_sem=sems.at[0, j], recv_sem=sems.at[1, j], device_id=sib, device_id_type=mesh_id)

    def mine(j):
        return pltpu.make_async_copy(uo_hbm.at[pl.ds(j * rows, rows)], own.at[j], o_sem.at[j])

    def theirs(j):
        return remote(us_hbm.at[pl.ds(j * rows, rows)], got.at[j], d_sem, j)

    half = uo_hbm.shape[1]
    quad = half // 2
    core = lax.rem(sp, 2)
    get_wv = pltpu.make_async_copy(wuv_hbm.at[:, pl.ds(pl.multiple_of(core * half, half), half)], wv, v_sem)
    get_wv.start()
    barrier = pltpu.get_barrier_semaphore()
    pl.semaphore_signal(barrier, inc=1, device_id=sib, device_id_type=mesh_id)
    for j in range(blocks):
        mine(j).start()
    pl.semaphore_wait(barrier, 1)
    cm = remote(m1_ref, mg, ml_sem, 0)
    cl = remote(l1_ref, lg, ml_sem, 1)
    cm.start()
    cl.start()
    for j in range(blocks):
        theirs(j).start()
    get_wv.wait()
    for p in range(2):
        wv_wide[...] = wv[:, p * quad:(p + 1) * quad, :].astype(jnp.float32)
        for h in range(quad):
            wvh[p * quad + h] = wv_wide[:, h, :].astype(jnp.bfloat16)
    ends = [pltpu.make_async_copy(wvh, wvh_hbm, v_sem), pltpu.make_async_copy(extra, send_hbm.at[blocks * rows // 2], e_sem)]
    ends[0].start()
    cm.wait()
    cl.wait()
    m0, m1 = m0_ref[...], mg[...]
    m = jnp.maximum(m0, m1)
    a0 = jnp.exp(m0 - m)
    a1 = jnp.exp(m1 - m)
    m_ref[...] = m
    l = l0_ref[...] * a0 + lg[...] * a1
    l_ref[...] = l
    extra[...] = jnp.concatenate([m, l, m, l], axis=1)
    lanes = lax.broadcasted_iota(jnp.int32, (1, 128), 1)

    def leave(j, out_hbm, first):
        return pltpu.make_async_copy(own.at[j], out_hbm.at[pl.ds(first, rows)], r_sem.at[j])

    def merge_block(j, out_hbm, first):
        mine(j).wait()
        theirs(j).wait_recv()
        for r in range(rows):
            hit = lanes == j * rows + r
            c0 = jnp.sum(jnp.where(hit, a0, 0.0), axis=1, keepdims=True)
            c1 = jnp.sum(jnp.where(hit, a1, 0.0), axis=1, keepdims=True)
            own[j, r] = own[j, r] * c0 + got[j, r] * c1
        leave(j, out_hbm, first).start()

    side = blocks // 2

    def body(j, carry):
        merge_block((1 - xpos) * side + j, send_hbm, j * rows)
        merge_block(xpos * side + j, keep_hbm, j * rows)
        return carry

    lax.fori_loop(0, side, body, 0)
    ends[1].start()

    def drain(j, carry):
        theirs(j).wait_send()
        leave(j, keep_hbm, 0).wait()
        return carry

    lax.fori_loop(0, blocks, drain, 0)
    for c in ends:
        c.wait()


def pair_merge(mo, lo, ms, ls, uo, us, w_uv, tag):
    count, half, rank = uo.shape
    vdim = w_uv.shape[2]
    rows = 8
    blocks = count // rows
    vmem = pl.BlockSpec(memory_space=pltpu.VMEM)
    any_spec = pl.BlockSpec(memory_space=pl.ANY)
    return pl.pallas_call(
        pair_kernel,
        in_specs=[vmem, vmem, vmem, vmem, any_spec, any_spec, any_spec],
        out_specs=[vmem, vmem, any_spec, any_spec, any_spec],
        out_shape=[
            *[jax.ShapeDtypeStruct((half, LANES), jnp.float32)] * 2,
            jax.ShapeDtypeStruct((count // 2, half, rank), jnp.float32),
            jax.ShapeDtypeStruct((count // 2 + 1, half, rank), jnp.float32),
            jax.ShapeDtypeStruct((half, rank, vdim), jnp.bfloat16),
        ],
        scratch_shapes=[
            pltpu.VMEM((blocks, rows, half, rank), jnp.float32),
            pltpu.VMEM((blocks, rows, half, rank), jnp.float32),
            pltpu.VMEM((half, LANES), jnp.float32),
            pltpu.VMEM((half, LANES), jnp.float32),
            pltpu.VMEM((rank, half, vdim), jnp.bfloat16),
            pltpu.VMEM((rank, half // 2, vdim), jnp.float32),
            pltpu.VMEM((half, rank, vdim), jnp.bfloat16),
            pltpu.VMEM((half, rank), jnp.float32),
            pltpu.SemaphoreType.DMA((2, 2)),
            pltpu.SemaphoreType.DMA((2, blocks)),
            pltpu.SemaphoreType.DMA((blocks,)),
            pltpu.SemaphoreType.DMA,
            pltpu.SemaphoreType.DMA((blocks,)),
            pltpu.SemaphoreType.DMA,
        ],
        compiler_params=pltpu.CompilerParams(collective_id=tag, has_side_effects=True, vmem_limit_bytes=VMEM_BYTES - 4 * VMEM_STEP),
        name='pair_merge_%d' % tag,
    )(mo, lo, ms, ls, uo, us, w_uv)


def merge_tiles(m0, l0, u0, m1, l1, u1):
    m = jnp.maximum(m0, m1)
    a0 = jnp.exp(m0 - m)
    a1 = jnp.exp(m1 - m)
    count = u0.shape[0]
    return m, l0 * a0 + l1 * a1, u0 * a0[:, :count].T[:, :, None] + u1 * a1[:, :count].T[:, :, None]


def solution(mesh):
    row_spec = P('dp', None)
    cache_spec = P('dp', 'sp', None)
    head_spec = P(None, 'tp', None)
    in_specs = (row_spec, cache_spec, cache_spec, P('dp'), P(), P(), P(), P(), head_spec, head_spec, head_spec, P('tp', None))
    out_specs = (row_spec, cache_spec, cache_spec)
    sibling = [(0, 1), (1, 0), (2, 3), (3, 2)]
    across = [(0, 2), (2, 0), (1, 3), (3, 1)]

    def local_step(hidden, lat_cache, rope_cache, positions, w_dq, gain_q, w_dkv, gain_kv, w_uq, w_uk, w_uv, w_out):
        rows = hidden.shape[0]
        slots = lat_cache.shape[1]
        heads = w_uq.shape[1]
        half = heads // 2
        scale = YARN_MSCALE ** 2 / math.sqrt(w_uq.shape[2])
        sp = lax.axis_index('sp')
        core = sp % 2
        xpos = sp // 2
        ids = jnp.arange(rows, dtype=jnp.int32)
        ahead = (positions[None, :] > positions[:, None]) | ((positions[None, :] == positions[:, None]) & (ids[None, :] < ids[:, None]))
        rank_of = jnp.sum(ahead.astype(jnp.int32), axis=1)
        pick = rank_of[None, :] == ids[:, None]
        order = jnp.sum(jnp.where(pick, ids[None, :], 0), axis=1)
        pos = jnp.sum(jnp.where(pick, positions[None, :], 0), axis=1)
        cos_t, sin_t = rope_tables(pos, rope_cache.shape[2])
        cos2 = jnp.concatenate([cos_t, cos_t], axis=1)
        sin2 = jnp.concatenate([sin_t, sin_t], axis=1)
        cq, latn, ropen = down_project(rank_of, hidden, w_dq, jnp.transpose(w_dkv), gain_q, gain_kv, cos2, sin2)
        rope_t = jnp.swapaxes(rope_cache, 1, 2)
        where = jnp.stack([sp * slots, core]).astype(jnp.int32)
        q_abs, q_rope = head_queries(cq, cos2, sin2, jnp.transpose(w_uq, (1, 2, 0)), w_uk)

        half_rows = rows // 2
        own_rows = rows // 4
        args = (scale, order, pos)
        uo, us, mo, lo, ms, ls, *held = attend_chunk(0, half_rows, *args, where, q_abs, q_rope, latn, ropen, lat_cache, rope_t, [])
        mk, lk, keep, send, wv_heads = pair_merge(mo, lo, ms, ls, uo, us, w_uv, 2)
        where, send = lax.optimization_barrier((where, send))
        ux = lax.ppermute(send, 'sp', across)
        uo, us, mo, lo, ms, ls, lat_out, rope_n = attend_chunk(half_rows, half_rows, *args, where, q_abs, q_rope, latn, ropen, lat_cache, rope_t, held)
        rope_out = jnp.swapaxes(rope_n, 1, 2)
        r = rank_of % half_rows
        x, k = r // own_rows, r % own_rows
        quarter = own_rows // 4
        c, t = k // (2 * quarter), (k // quarter) % 2
        place = (rank_of // half_rows) * half_rows + ((x * 2 + c) * 2 + t) * quarter + k % quarter
        place = place.astype(jnp.int32)

        def far(_, second):
            m0, l0, m1, l1, u0, u1 = second
            gm0, gl0, gm1, gl1, gu0, gu1 = lax.ppermute(second, 'sp', across)
            m0, l0, u0 = merge_tiles(m0, l0, u0, gm0, gl0, gu0)
            m1, l1, u1 = merge_tiles(m1, l1, u1, gm1, gl1, gu1)
            return m0, l0, m1, l1, u0, u1

        trips = (pos[half_rows] >= 2 * slots).astype(jnp.int32)
        ux, uo = lax.optimization_barrier((ux, uo))
        second = lax.fori_loop(0, trips, far, (mo, lo, ms, ls, uo, us))
        out = finish(place, (mk, lk, keep, ux), second, hidden, wv_heads, w_out, 12, 3)
        return out, lat_out, rope_out

    return jax.shard_map(local_step, mesh=mesh, in_specs=in_specs, out_specs=out_specs, check_vma=False)
```
